1024 devices in a mesh: grp: 16 (over y, x), wide: 64 (over z, core).
Axes of the slice: x: 4, y: 4, z: 32, core: 2. Of those that a mesh axis runs over, the one named last changes fastest.
Arguments:
- sequences: bfloat16 [1024, 128, 512], P(('grp', 'wide')), may hold values from -6 to 6
- upstream: bfloat16 [1024, 128, 512], P(('grp', 'wide')), may hold values from -6 to 6
- lengths: int32 [16, 64, 1], P('grp'), may hold values from 16 to 128
- swap_table: int32 [16, 32, 1], P('grp'), may hold values from 0 to 1
- input_weight: bfloat16 [512, 2048], replicated, may hold values from -0.25 to 0.25
- output_weight: bfloat16 [512, 512], replicated, may hold values from -0.25 to 0.25
Outputs:
- layer_out: bfloat16 [1024, 128, 512], P(('grp', 'wide'))
- input_grad: bfloat16 [1024, 128, 512], P(('grp', 'wide'))
- input_weight_gradient: float32 [512, 2048], P('wide')
- output_weight_gradient: float32 [512, 512], P('wide')
The draws below stay inside these ranges and needn't reach their ends.
All inputs are finite; a program needn't handle non-finite values.
Results may differ from the reference program's by a relative error of at most 0.018.
Values may be sent and summed in bfloat16 or wider, within the bound.
No kernel may reach another device: no remote copies, remote signals or barrier semaphores. Data moves between devices by JAX's collectives and lax.ppermute only.
A program may use at most 64 MiB of HBM per device.

```python
import jax
import jax.numpy as jnp
from jax import lax

HEADS = 8
HEAD_DIM = 64
D = 512
SEQ_DEV = 1
LEN = 128
SEQS = 1024
N_GRP = 16
N_WIDE = 64


def with_ends(values, own_key, least, top_value):
    place = [jax.random.randint(jax.random.fold_in(own_key, axis), (), 0, length) for axis, length in enumerate(values.shape)]
    main_axis = values.shape.index(max(values.shape))
    next_to = place[:main_axis] + [(place[main_axis] + 1) % values.shape[main_axis]] + place[main_axis + 1:]
    return values.at[tuple(place)].set(least).at[tuple(next_to)].set(top_value)


def block_levels(rng, extent, pieces, low, top_value):
    factor_of = 1.0
    for position, shards_of in pieces:
        heights = jax.random.uniform(jax.random.fold_in(jax.random.fold_in(rng, 6), position), (shards_of,), jnp.float32, low / len(pieces), top_value / len(pieces))
        factor_of = factor_of * jnp.repeat(jnp.exp(heights), extent[position] // shards_of).reshape((-1,) + (1,) * (len(extent) - 1 - position))
    return factor_of


def centred(rng, shape, scale, bound, pieces=(), kind=jnp.bfloat16):
    gain = block_levels(rng, shape, pieces, -0.22, 0.18) if pieces else 1.0
    drawn = jax.random.normal(rng, shape, jnp.float32) * scale * gain
    return jnp.minimum(jnp.maximum(drawn, -bound), bound).astype(kind)


def setup_inputs(seed: int = 0) -> dict:
    key_of = jax.random.split(jax.random.key(seed), 7)
    sequences = centred(key_of[0], (SEQS, LEN, D), 1.0, 6.0, ((0, 1024),))
    upstream = centred(key_of[1], (SEQS, LEN, D), 1.0, 6.0, ((0, 1024),))
    lengths = with_ends(jax.random.randint(key_of[2], (N_GRP, N_WIDE, SEQ_DEV), max(1, LEN // 8), LEN + 1), jax.random.fold_in(key_of[2], 1), max(1, LEN // 8), LEN).astype(jnp.int32)
    swap_table = with_ends(jax.random.randint(key_of[3], (N_GRP, N_WIDE // 2, SEQ_DEV), 0, 2), jax.random.fold_in(key_of[3], 1), 0, 1).astype(jnp.int32)
    input_weight = centred(key_of[4], (D, 4 * D), D ** -0.5, 0.25)
    output_weight = centred(key_of[5], (D, D), D ** -0.5, 0.25)
    return {"sequences": sequences, "upstream": upstream, "lengths": lengths, "swap_table": swap_table, "input_weight": input_weight, "output_weight": output_weight}


epsilon = 1e-06

def normalize(values):
    return values * lax.rsqrt(lax.optimization_barrier(jnp.mean(values * values, axis=-1, keepdims=True)) + epsilon)

def layer_grads(rows, cotangent, lengths, input_weight, output_weight):
    slots, length_rows, width = rows.shape
    positions = jnp.arange(length_rows, dtype=jnp.int32)
    valid_rows = positions[None, :] < lengths[:, None]
    allowed = (positions[:, None] >= positions[None, :])[None, None] & valid_rows[:, None, None, :]
    input_single_precision = rows.astype(jnp.float32)
    norm_result_input = normalize(input_single_precision).astype(jnp.bfloat16)
    hidden_state = jnp.einsum('xbg,gm->xbm', norm_result_input.astype(jnp.float32), input_weight.astype(jnp.float32))

    def post(hidden_state, input_single_precision):
        activated = jax.nn.silu(hidden_state).astype(jnp.bfloat16)
        gate_part = activated[..., :width]
        value_part = activated[..., width:2 * width].reshape(slots, length_rows, HEADS, HEAD_DIM)
        query_part = activated[..., 2 * width:3 * width].reshape(slots, length_rows, HEADS, HEAD_DIM)
        key_part = activated[..., 3 * width:].reshape(slots, length_rows, HEADS, HEAD_DIM)
        scores = jnp.einsum('sqhc,skhc->shqk', query_part.astype(jnp.float32), key_part.astype(jnp.float32)) * HEAD_DIM ** (-0.5)
        weights = jnp.where(allowed, jax.nn.silu(scores), 0.0).astype(jnp.bfloat16)
        attended = jnp.einsum('shqk,skhc->sqhc', weights.astype(jnp.float32), value_part.astype(jnp.float32)).reshape(slots, length_rows, width)
        gate_applied = (gate_part * normalize(attended)).astype(jnp.bfloat16)
        layer_result = input_single_precision + jnp.einsum('xbg,gm->xbm', gate_applied.astype(jnp.float32), output_weight.astype(jnp.float32))
        return (layer_result.astype(jnp.bfloat16), gate_applied)
    layer_result, pull_back, gate_applied = jax.vjp(post, hidden_state, input_single_precision, has_aux=True)
    mask_applied = cotangent * valid_rows[..., None].astype(cotangent.dtype)
    hidden_state_gradient, direct_grad = pull_back(mask_applied)
    hidden_state_gradient = hidden_state_gradient.astype(jnp.bfloat16)
    norm_result_gradient = jnp.einsum('wmo,bo->wmb', hidden_state_gradient.astype(jnp.float32), input_weight.astype(jnp.float32))
    _, norm_back = jax.vjp(normalize, input_single_precision)
    input_grad = (direct_grad + norm_back(norm_result_gradient)[0]).astype(jnp.bfloat16)
    input_weight_gradient = jnp.einsum('uwn,uwo->no', norm_result_input.astype(jnp.float32), hidden_state_gradient.astype(jnp.float32))
    output_weight_gradient = jnp.einsum('uwn,uwo->no', gate_applied.astype(jnp.float32), mask_applied.astype(jnp.float32))
    return (layer_result, input_grad, input_weight_gradient, output_weight_gradient)

def reference(sequences, upstream, lengths, swap_table, input_weight, output_weight):
    group_rows = sequences.reshape(N_GRP, N_WIDE * SEQ_DEV, LEN, D)
    group_cts = upstream.reshape(N_GRP, N_WIDE * SEQ_DEV, LEN, D)
    group_lens = lengths.reshape(N_GRP, N_WIDE * SEQ_DEV).astype(jnp.int32)

    def step(carry, item):
        rows, cotangent, lens = item
        layer_result, input_grad, input_weight_gradient, output_weight_gradient = layer_grads(rows, cotangent, lens, input_weight, output_weight)
        return ((carry[0] + input_weight_gradient, carry[1] + output_weight_gradient), (layer_result, input_grad))
    start = (jnp.zeros((D, 4 * D), jnp.float32), jnp.zeros((D, D), jnp.float32))
    totals, results = lax.scan(step, start, (group_rows, group_cts, group_lens))
    outputs = results[0].reshape(N_GRP, N_WIDE, SEQ_DEV, LEN, D)
    partner = jnp.roll(outputs, N_WIDE // 2, axis=1)
    swap_flags = jnp.concatenate([swap_table, swap_table], axis=1)
    layer_out = jnp.where((swap_flags == 1)[..., None, None], partner, outputs).reshape(SEQS, LEN, D)
    input_grad = results[1].reshape(SEQS, LEN, D)
    grad_scale = (SEQS * LEN) ** (-0.5)
    return (layer_out, input_grad, totals[0] * grad_scale, totals[1] * grad_scale)
```

```python
import math

import jax
import jax.numpy as jnp
from jax import lax
from jax.experimental import pallas as pl
from jax.experimental.pallas import tpu as pltpu
from jax.sharding import PartitionSpec as P

HEADS = 8
HEAD_DIM = 64
LEN = 128
D = 512
GROUPS = 16
CHIPS = 32
CORES = 2
ROWS = 320
epsilon = 1e-06
f32 = jnp.float32
bf16 = jnp.bfloat16


def nn(a, b):
    return lax.dot_general(a, b, (((1,), (0,)), ((), ())), preferred_element_type=f32)


def nt(a, b):
    return lax.dot_general(a, b, (((1,), (1,)), ((), ())), preferred_element_type=f32)


def tn(a, b):
    return lax.dot_general(a, b, (((0,), (0,)), ((), ())), preferred_element_type=f32)


def sigmoid(x):
    return 0.5 * jnp.tanh(0.5 * x) + 0.5


def layer_kernel(
    lengths_ref,
    x_ref,
    up_ref,
    win_ref,
    wout_ref,
    home_ref,
    xgrad_ref,
    send_ref,
    keep_ref,
    act_ref,
    slope_ref,
    wslope_ref,
    weights_ref,
    hgrad_ref,
    normed_t,
    gated_t,
):
    position = lax.axis_index("wide")
    length = lengths_ref[position]
    core = lax.rem(position, 2)
    x = x_ref[0].astype(f32)
    inverse = lax.rsqrt(jnp.mean(x * x, axis=-1, keepdims=True) + epsilon)
    unit = x * inverse
    normed = unit.astype(bf16)
    normed_t[...] = unit.astype(bf16).astype(f32).T.reshape(CHIPS, 16, LEN)
    for part in range(4):
        columns = pl.ds(part * D, D)
        hidden = nn(normed, win_ref[:, columns])
        sig = sigmoid(hidden)
        activated = hidden * sig
        act_ref[:, columns] = activated.astype(bf16)
        slope_ref[:, columns] = sig + activated * (1.0 - sig)

    query_at = lax.broadcasted_iota(jnp.int32, (LEN, LEN), 0)
    key_at = lax.broadcasted_iota(jnp.int32, (LEN, LEN), 1)
    allowed = (key_at <= query_at) & (key_at < length)
    first = lax.broadcasted_iota(jnp.int32, (LEN, LEN), 1) < HEAD_DIM

    def by_head(block):
        wide = block.astype(f32)
        return (
            jnp.where(first, wide, 0.0).astype(bf16),
            jnp.where(first, 0.0, wide).astype(bf16),
        )

    attended = []
    for pair in range(HEADS // 2):
        at = pair * 128
        queries = by_head(act_ref[:, 2 * D + at : 2 * D + at + 128])
        keys = act_ref[:, 3 * D + at : 3 * D + at + 128]
        values = by_head(act_ref[:, D + at : D + at + 128])
        for side in range(2):
            scores = nt(queries[side], keys) * HEAD_DIM**-0.5
            sig = sigmoid(scores)
            smooth = scores * sig
            slope = (sig + smooth * (1.0 - sig)) * HEAD_DIM**-0.5
            wslope_ref[2 * pair + side] = jnp.where(allowed, slope, 0.0)
            weights_ref[pair, side * LEN : (side + 1) * LEN, :] = jnp.where(
                allowed, smooth, 0.0
            ).astype(bf16)
        attended.append(
            nn(weights_ref[pair, :LEN, :], values[0]) + nn(weights_ref[pair, LEN:, :], values[1])
        )
    attended = jnp.concatenate(attended, axis=1)
    spread = lax.rsqrt(jnp.mean(attended * attended, axis=-1, keepdims=True) + epsilon)
    unit_attended = attended * spread
    gate = act_ref[:, :D].astype(f32)
    gated = (gate * unit_attended).astype(bf16)
    gated_t[...] = gated.astype(f32).T
    home_ref[0] = (x + nn(gated, wout_ref[...])).astype(bf16)

    alive = lax.broadcasted_iota(jnp.int32, (LEN, D), 0) < length
    masked_wide = jnp.where(alive, up_ref[0].astype(f32), 0.0)
    masked = masked_wide.astype(bf16)
    gated_grad = nt(masked, wout_ref[...]).astype(bf16).astype(f32)
    hgrad_ref[:, :D] = (
        (gated_grad * unit_attended).astype(bf16).astype(f32) * slope_ref[:, :D]
    ).astype(bf16)
    unit_grad = gated_grad * gate
    overlap = jnp.mean(unit_grad * unit_attended, axis=-1, keepdims=True)
    attended_grad = spread * (unit_grad - unit_attended * overlap)

    for pair in range(HEADS // 2):
        at = pair * 128
        queries = by_head(act_ref[:, 2 * D + at : 2 * D + at + 128])
        keys = by_head(act_ref[:, 3 * D + at : 3 * D + at + 128])
        values = act_ref[:, D + at : D + at + 128]
        grads = by_head(attended_grad[:, at : at + 128])
        both = jnp.concatenate(grads, axis=0)
        weight_grads = nt(both, values)
        value_grad = tn(weights_ref[pair], both)
        score_grads = (
            weight_grads * wslope_ref[2 * pair : 2 * pair + 2].reshape(2 * LEN, LEN)
        ).astype(bf16)
        query_grad = nn(score_grads[:LEN], keys[0]) + nn(score_grads[LEN:], keys[1])
        key_grad = tn(score_grads, jnp.concatenate(queries, axis=0))
        for start, grad in ((D, value_grad), (2 * D, query_grad), (3 * D, key_grad)):
            columns = pl.ds(start + at, 128)
            hgrad_ref[:, columns] = (grad * slope_ref[:, columns]).astype(bf16)

    unit_grad = nt(hgrad_ref[...], win_ref[...])
    overlap = jnp.mean(unit_grad * unit, axis=-1, keepdims=True)
    xgrad_ref[0] = (masked_wide + inverse * (unit_grad - unit * overlap)).astype(bf16)

    for out_ref, side in ((send_ref, 1 - core), (keep_ref, core)):
        mine = normed_t[:, pl.ds(pl.multiple_of(side * 8, 8), 8), :].reshape(256, LEN).astype(bf16)
        for block in range(4):
            grads = nn(mine, hgrad_ref[:, block * 512 : (block + 1) * 512]).astype(bf16)
            for j in range(4):
                out_ref[4 * block + j, 0:256, :] = grads[:, j * 128 : (j + 1) * 128]
        mine = jnp.concatenate(
            [gated_t[pl.ds(side * 8 + i, CHIPS, stride=16), :] for i in range(8)], axis=0
        ).astype(bf16)
        grads = nn(mine, masked).astype(bf16)
        for block in range(4):
            for p in range(4):
                out_ref[4 * block + p, 256:320, :] = grads[
                    p * 64 : (p + 1) * 64, block * 128 : (block + 1) * 128
                ]


def layer(lengths, x, up, win, wout):
    vmem = pl.BlockSpec(memory_space=pltpu.VMEM)
    smem = pl.BlockSpec(memory_space=pltpu.SMEM)
    block = jax.ShapeDtypeStruct((1, LEN, D), bf16)
    grads = jax.ShapeDtypeStruct((GROUPS, ROWS, 128), bf16)
    return pl.pallas_call(
        layer_kernel,
        out_shape=(block, block, grads, grads),
        in_specs=[smem, vmem, vmem, vmem, vmem],
        out_specs=(vmem, vmem, vmem, vmem),
        scratch_shapes=[
            pltpu.VMEM((LEN, 4 * D), bf16),
            pltpu.VMEM((LEN, 4 * D), f32),
            pltpu.VMEM((HEADS, LEN, LEN), f32),
            pltpu.VMEM((HEADS // 2, 2 * LEN, LEN), bf16),
            pltpu.VMEM((LEN, 4 * D), bf16),
            pltpu.VMEM((CHIPS, 16, LEN), f32),
            pltpu.VMEM((D, LEN), f32),
        ],
        compiler_params=pltpu.CompilerParams(vmem_limit_bytes=40 << 20),
        name="layer",
    )(lengths, x, up, win, wout)


def group_sum_kernel(parts_ref, out_ref, total):
    summed = parts_ref[0].astype(f32)
    for g in range(1, GROUPS):
        summed += parts_ref[g].astype(f32)
    total[...] = summed
    for z in range(CHIPS):
        out_ref[z, 0:8, :] = total[8 * z : 8 * z + 8, :].astype(bf16)
        out_ref[z, 8:10, :] = total[pl.ds(256 + z, 2, stride=CHIPS), :].astype(bf16)


def group_sum(parts):
    vmem = pl.BlockSpec(memory_space=pltpu.VMEM)
    return pl.pallas_call(
        group_sum_kernel,
        out_shape=jax.ShapeDtypeStruct((CHIPS, 10, 128), bf16),
        in_specs=[vmem],
        out_specs=vmem,
        scratch_shapes=[pltpu.VMEM((ROWS, 128), f32)],
        name="group_sum",
    )(parts)


def chip_sum_kernel(parts_ref, out_ref):
    summed = parts_ref[0].astype(f32)
    for z in range(1, CHIPS):
        summed += parts_ref[z].astype(f32)
    summed = summed.astype(bf16)
    for g in range(GROUPS):
        out_ref[g] = summed


def chip_sum(parts):
    vmem = pl.BlockSpec(memory_space=pltpu.VMEM)
    return pl.pallas_call(
        chip_sum_kernel,
        out_shape=jax.ShapeDtypeStruct((GROUPS, 10, 128), bf16),
        in_specs=[vmem],
        out_specs=vmem,
        name="chip_sum",
    )(parts)


def finish_kernel(scale, swap_ref, home_ref, arrived_ref, parts_ref, out_ref, din_ref, dout_ref):
    position = lax.axis_index("wide")
    chosen = swap_ref[lax.rem(position, CHIPS)] == 1

    @pl.when(chosen)
    def _():
        out_ref[...] = arrived_ref[...]

    @pl.when(jnp.logical_not(chosen))
    def _():
        out_ref[...] = home_ref[...]

    for g in range(GROUPS):
        piece = parts_ref[g].astype(f32) * scale
        din_ref[:, g * 128 : (g + 1) * 128] = piece[:8]
        block, pair = g // 4, g % 4
        dout_ref[2 * pair : 2 * pair + 2, block * 128 : (block + 1) * 128] = piece[8:10]


def finish(scale, swaps, home, arrived, parts):
    vmem = pl.BlockSpec(memory_space=pltpu.VMEM)
    smem = pl.BlockSpec(memory_space=pltpu.SMEM)
    return pl.pallas_call(
        lambda *refs: finish_kernel(scale, *refs),
        out_shape=(
            jax.ShapeDtypeStruct((1, LEN, D), bf16),
            jax.ShapeDtypeStruct((8, 4 * D), f32),
            jax.ShapeDtypeStruct((8, D), f32),
        ),
        in_specs=[smem, vmem, vmem, vmem],
        out_specs=(vmem, vmem, vmem),
        name="finish",
    )(swaps, home, arrived, parts)


def body(sequences, upstream, lengths, swap_table, input_weight, output_weight):
    wide = lax.axis_size("wide")
    half = wide // 2
    home, input_grad, send, keep = layer(
        lengths.reshape(wide), sequences, upstream, input_weight, output_weight
    )
    received = lax.ppermute(send, "wide", [(i, i ^ 1) for i in range(wide)])
    arrived = lax.ppermute(home, "wide", [(i, (i + half) % wide) for i in range(wide)])
    chip = (keep.astype(f32) + received.astype(f32)).astype(bf16)
    parts = lax.all_to_all(chip, "grp", 0, 0, tiled=True)
    same_core = [[2 * z + c for z in range(CHIPS)] for c in range(CORES)]
    parts = lax.all_to_all(
        group_sum(parts), "wide", 0, 0, tiled=True, axis_index_groups=same_core
    )
    parts = lax.all_to_all(chip_sum(parts), "grp", 0, 0, tiled=True)
    scale = 1.0 / math.sqrt(LEN * wide * lax.axis_size("grp"))
    layer_out, total_in, total_out = finish(
        scale, swap_table.reshape(half), home, arrived, parts
    )
    return (layer_out, input_grad, total_in, total_out)


def solution(mesh):
    placed = (
        P(("grp", "wide"), None, None),
        P(("grp", "wide"), None, None),
        P("grp", None, None),
        P("grp", None, None),
        P(),
        P(),
    )
    return jax.shard_map(
        body,
        mesh=mesh,
        in_specs=placed,
        out_specs=(
            P(("grp", "wide"), None, None),
            P(("grp", "wide"), None, None),
            P("wide", None),
            P("wide", None),
        ),
        check_vma=False,
    )
```

```python
import math

import jax
import jax.numpy as jnp
from jax import lax
from jax.experimental import pallas as pl
from jax.experimental.pallas import tpu as pltpu
from jax.sharding import PartitionSpec as P


HEADS = 8
HEAD_DIM = 64
LEN = 128
D = 512
GROUPS = 16
CHIPS = 32
CORES = 2
ROWS = 320
PIECE = 10
epsilon = 1e-06
f32 = jnp.float32
bf16 = jnp.bfloat16


def nn(a, b):
    return lax.dot_general(a, b, (((1,), (0,)), ((), ())), preferred_element_type=f32)


def nt(a, b):
    return lax.dot_general(a, b, (((1,), (1,)), ((), ())), preferred_element_type=f32)


def tn(a, b):
    return lax.dot_general(a, b, (((0,), (0,)), ((), ())), preferred_element_type=f32)


def sigmoid(x):
    return 0.5 * jnp.tanh(0.5 * x) + 0.5


def layer_kernel(
    lengths_hbm,
    x_hbm,
    up_hbm,
    win_hbm,
    wout_hbm,
    home_ref,
    xgrad_ref,
    send_ref,
    keep_ref,
    act_ref,
    slope_ref,
    wslope_ref,
    weights_ref,
    hgrad_ref,
    normed_t,
    gated_t,
    lengths_ref,
    x_ref,
    up_ref,
    win_ref,
    wout_ref,
    arrivals,
):
    parts = [(x_hbm.at[0], x_ref)]
    parts += [(win_hbm.at[:, pl.ds(j * D, D)], win_ref.at[:, pl.ds(j * D, D)]) for j in range(4)]
    parts += [(lengths_hbm, lengths_ref), (wout_hbm, wout_ref), (up_hbm.at[0], up_ref)]
    copies = [
        pltpu.make_async_copy(src, dst, arrivals.at[i]) for i, (src, dst) in enumerate(parts)
    ]
    for copy in copies:
        copy.start()
    position = lax.axis_index("wide")
    core = lax.rem(position, 2)
    copies[0].wait()
    x = x_ref[...].astype(f32)
    inverse = lax.rsqrt(jnp.mean(x * x, axis=-1, keepdims=True) + epsilon)
    unit = x * inverse
    normed = unit.astype(bf16)
    normed_t[...] = unit.astype(bf16).astype(f32).T.reshape(CHIPS, 16, LEN)
    for part in range(4):
        columns = pl.ds(part * D, D)
        copies[1 + part].wait()
        hidden = nn(normed, win_ref[:, columns])
        sig = sigmoid(hidden)
        activated = hidden * sig
        act_ref[:, columns] = activated.astype(bf16)
        slope_ref[:, columns] = sig + activated * (1.0 - sig)

    copies[5].wait()
    length = lengths_ref[position]
    query_at = lax.broadcasted_iota(jnp.int32, (LEN, LEN), 0)
    key_at = lax.broadcasted_iota(jnp.int32, (LEN, LEN), 1)
    allowed = (key_at <= query_at) & (key_at < length)
    first = lax.broadcasted_iota(jnp.int32, (LEN, LEN), 1) < HEAD_DIM

    def by_head(block):
        wide = block.astype(f32)
        return (
            jnp.where(first, wide, 0.0).astype(bf16),
            jnp.where(first, 0.0, wide).astype(bf16),
        )

    attended = []
    for pair in range(HEADS // 2):
        at = pair * 128
        queries = by_head(act_ref[:, 2 * D + at : 2 * D + at + 128])
        keys = act_ref[:, 3 * D + at : 3 * D + at + 128]
        values = by_head(act_ref[:, D + at : D + at + 128])
        for side in range(2):
            scores = nt(queries[side], keys) * HEAD_DIM**-0.5
            sig = sigmoid(scores)
            smooth = scores * sig
            slope = (sig + smooth * (1.0 - sig)) * HEAD_DIM**-0.5
            wslope_ref[2 * pair + side] = jnp.where(allowed, slope, 0.0)
            weights_ref[pair, side * LEN : (side + 1) * LEN, :] = jnp.where(
                allowed, smooth, 0.0
            ).astype(bf16)
        attended.append(
            nn(weights_ref[pair, :LEN, :], values[0]) + nn(weights_ref[pair, LEN:, :], values[1])
        )
    attended = jnp.concatenate(attended, axis=1)
    spread = lax.rsqrt(jnp.mean(attended * attended, axis=-1, keepdims=True) + epsilon)
    unit_attended = attended * spread
    gate = act_ref[:, :D].astype(f32)
    gated = (gate * unit_attended).astype(bf16)
    gated_t[...] = gated.astype(f32).T
    copies[6].wait()
    home_ref[0] = (x + nn(gated, wout_ref[...])).astype(bf16)

    copies[7].wait()
    alive = lax.broadcasted_iota(jnp.int32, (LEN, D), 0) < length
    masked_wide = jnp.where(alive, up_ref[...].astype(f32), 0.0)
    masked = masked_wide.astype(bf16)
    gated_grad = nt(masked, wout_ref[...]).astype(bf16).astype(f32)
    hgrad_ref[:, :D] = (
        (gated_grad * unit_attended).astype(bf16).astype(f32) * slope_ref[:, :D]
    ).astype(bf16)
    unit_grad = gated_grad * gate
    overlap = jnp.mean(unit_grad * unit_attended, axis=-1, keepdims=True)
    attended_grad = spread * (unit_grad - unit_attended * overlap)

    for pair in range(HEADS // 2):
        at = pair * 128
        queries = by_head(act_ref[:, 2 * D + at : 2 * D + at + 128])
        keys = by_head(act_ref[:, 3 * D + at : 3 * D + at + 128])
        values = act_ref[:, D + at : D + at + 128]
        grads = by_head(attended_grad[:, at : at + 128])
        both = jnp.concatenate(grads, axis=0)
        weight_grads = nt(both, values)
        value_grad = tn(weights_ref[pair], both)
        score_grads = (
            weight_grads * wslope_ref[2 * pair : 2 * pair + 2].reshape(2 * LEN, LEN)
        ).astype(bf16)
        query_grad = nn(score_grads[:LEN], keys[0]) + nn(score_grads[LEN:], keys[1])
        key_grad = tn(score_grads, jnp.concatenate(queries, axis=0))
        for start, grad in ((D, value_grad), (2 * D, query_grad), (3 * D, key_grad)):
            columns = pl.ds(start + at, 128)
            hgrad_ref[:, columns] = (grad * slope_ref[:, columns]).astype(bf16)

    unit_grad = nt(hgrad_ref[...], win_ref[...])
    overlap = jnp.mean(unit_grad * unit, axis=-1, keepdims=True)
    xgrad_ref[0] = (masked_wide + inverse * (unit_grad - unit * overlap)).astype(bf16)

    for out_ref, side in ((send_ref, 1 - core), (keep_ref, core)):
        mine = normed_t[:, pl.ds(pl.multiple_of(side * 8, 8), 8), :].reshape(256, LEN).astype(bf16)
        for block in range(4):
            grads = nn(mine, hgrad_ref[:, block * 512 : (block + 1) * 512]).astype(bf16)
            for j in range(4):
                out_ref[4 * block + j, 0:256, :] = grads[:, j * 128 : (j + 1) * 128]
        mine = jnp.concatenate(
            [gated_t[pl.ds(side * 8 + i, CHIPS, stride=16), :] for i in range(8)], axis=0
        ).astype(bf16)
        grads = nn(mine, masked).astype(bf16)
        for block in range(4):
            for p in range(4):
                out_ref[4 * block + p, 256:320, :] = grads[
                    p * 64 : (p + 1) * 64, block * 128 : (block + 1) * 128
                ]


def kept_in(space, *arrays):
    return [pltpu.with_memory_space_constraint(array, space) for array in arrays]


def layer(lengths, x, up, win, wout):
    vmem = pl.BlockSpec(memory_space=pltpu.VMEM)
    hbm = pl.BlockSpec(memory_space=pltpu.HBM)
    block = jax.ShapeDtypeStruct((1, LEN, D), bf16)
    grads = jax.ShapeDtypeStruct((GROUPS, ROWS, 128), bf16)
    return pl.pallas_call(
        layer_kernel,
        out_shape=(block, block, grads, grads),
        in_specs=[hbm] * 5,
        out_specs=(vmem, vmem, vmem, vmem),
        scratch_shapes=[
            pltpu.VMEM((LEN, 4 * D), bf16),
            pltpu.VMEM((LEN, 4 * D), f32),
            pltpu.VMEM((HEADS, LEN, LEN), f32),
            pltpu.VMEM((HEADS // 2, 2 * LEN, LEN), bf16),
            pltpu.VMEM((LEN, 4 * D), bf16),
            pltpu.VMEM((CHIPS, 16, LEN), f32),
            pltpu.VMEM((D, LEN), f32),
            pltpu.SMEM((2 * CHIPS,), jnp.int32),
            pltpu.VMEM((LEN, D), bf16),
            pltpu.VMEM((LEN, D), bf16),
            pltpu.VMEM((D, 4 * D), bf16),
            pltpu.VMEM((D, D), bf16),
            pltpu.SemaphoreType.DMA((8,)),
        ],
        compiler_params=pltpu.CompilerParams(vmem_limit_bytes=40 << 20),
        name="layer",
    )(*kept_in(pltpu.HBM, lengths, x, up, win, wout))


def group_sum_kernel(parts_ref, out_ref, total, ordered):
    summed = parts_ref[0].astype(f32)
    for g in range(1, GROUPS):
        summed += parts_ref[g].astype(f32)
    total[...] = summed
    for z in range(CHIPS):
        ordered[PIECE * z : PIECE * z + 8, :] = total[8 * z : 8 * z + 8, :]
        ordered[PIECE * z + 8 : PIECE * z + 10, :] = total[pl.ds(256 + z, 2, stride=CHIPS), :]
    out_ref[...] = ordered[...].astype(bf16)


def group_sum(parts):
    vmem = pl.BlockSpec(memory_space=pltpu.VMEM)
    return pl.pallas_call(
        group_sum_kernel,
        out_shape=jax.ShapeDtypeStruct((CHIPS * PIECE, 128), bf16),
        in_specs=[vmem],
        out_specs=vmem,
        scratch_shapes=[pltpu.VMEM((ROWS, 128), f32), pltpu.VMEM((CHIPS * PIECE, 128), f32)],
        name="group_sum",
    )(*kept_in(pltpu.VMEM, parts))


def chip_sum_kernel(parts_ref, out_ref, parts, copies):
    parts[...] = parts_ref[...].astype(f32)
    summed = parts[0:PIECE, :]
    for z in range(1, CHIPS):
        summed += parts[PIECE * z : PIECE * (z + 1), :]
    for g in range(GROUPS):
        copies[PIECE * g : PIECE * (g + 1), :] = summed
    out_ref[...] = copies[...].astype(bf16)


def chip_sum(parts):
    vmem = pl.BlockSpec(memory_space=pltpu.VMEM)
    return pl.pallas_call(
        chip_sum_kernel,
        out_shape=jax.ShapeDtypeStruct((GROUPS * PIECE, 128), bf16),
        in_specs=[vmem],
        out_specs=vmem,
        scratch_shapes=[
            pltpu.VMEM((CHIPS * PIECE, 128), f32),
            pltpu.VMEM((GROUPS * PIECE, 128), f32),
        ],
        name="chip_sum",
    )(*kept_in(pltpu.VMEM, parts))


def finish_kernel(
    scale, swap_ref, home_ref, arrived_ref, parts_ref, out_ref, din_ref, dout_ref, parts
):
    position = lax.axis_index("wide")
    chosen = swap_ref[lax.rem(position, CHIPS)] == 1

    @pl.when(chosen)
    def _():
        out_ref[...] = arrived_ref[...]

    @pl.when(jnp.logical_not(chosen))
    def _():
        out_ref[...] = home_ref[...]

    parts[...] = parts_ref[...].astype(f32) * scale
    for g in range(GROUPS):
        din_ref[:, g * 128 : (g + 1) * 128] = parts[PIECE * g : PIECE * g + 8, :]
        block, pair = g // 4, g % 4
        dout_ref[2 * pair : 2 * pair + 2, block * 128 : (block + 1) * 128] = parts[
            PIECE * g + 8 : PIECE * g + 10, :
        ]


def finish(scale, swaps, home, arrived, parts):
    vmem = pl.BlockSpec(memory_space=pltpu.VMEM)
    smem = pl.BlockSpec(memory_space=pltpu.SMEM)
    return pl.pallas_call(
        lambda *refs: finish_kernel(scale, *refs),
        out_shape=(
            jax.ShapeDtypeStruct((1, LEN, D), bf16),
            jax.ShapeDtypeStruct((8, 4 * D), f32),
            jax.ShapeDtypeStruct((8, D), f32),
        ),
        in_specs=[smem, vmem, vmem, vmem],
        out_specs=(vmem, vmem, vmem),
        scratch_shapes=[pltpu.VMEM((GROUPS * PIECE, 128), f32)],
        name="finish",
    )(swaps, *kept_in(pltpu.VMEM, home, arrived, parts))


def exchanged(rows, count, axis, groups=None):
    pieces = rows.reshape(count, PIECE // 2, 2, 128)
    pieces = lax.all_to_all(pieces, axis, 0, 0, tiled=True, axis_index_groups=groups)
    return pieces.reshape(count * PIECE, 128)


def body(sequences, upstream, lengths, swap_table, input_weight, output_weight):
    wide = lax.axis_size("wide")
    half = wide // 2
    home, input_grad, send, keep = layer(
        lengths.reshape(wide), sequences, upstream, input_weight, output_weight
    )
    received = lax.ppermute(send, "wide", [(i, i ^ 1) for i in range(wide)])
    arrived = lax.ppermute(home, "wide", [(i, (i + half) % wide) for i in range(wide)])
    chip = (keep.astype(f32) + received.astype(f32)).astype(bf16)
    parts = lax.all_to_all(chip, "grp", 0, 0, tiled=True)
    same_core = [[2 * z + c for z in range(CHIPS)] for c in range(CORES)]
    parts = group_sum(parts)
    parts = exchanged(parts, CHIPS, "wide", same_core)
    parts = exchanged(chip_sum(parts), GROUPS, "grp")
    scale = 1.0 / math.sqrt(LEN * wide * lax.axis_size("grp"))
    layer_out, total_in, total_out = finish(
        scale, swap_table.reshape(half), home, arrived, parts
    )
    return (layer_out, input_grad, total_in, total_out)


def solution(mesh):
    placed = (
        P(("grp", "wide"), None, None),
        P(("grp", "wide"), None, None),
        P("grp", None, None),
        P("grp", None, None),
        P(),
        P(),
    )
    return jax.shard_map(
        body,
        mesh=mesh,
        in_specs=placed,
        out_specs=(
            P(("grp", "wide"), None, None),
            P(("grp", "wide"), None, None),
            P("wide", None),
            P("wide", None),
        ),
        check_vma=False,
    )
```

```python
import math

import jax
import jax.numpy as jnp
from jax import lax
from jax.experimental import pallas as pl
from jax.experimental.pallas import tpu as pltpu
from jax.sharding import PartitionSpec as P


HEADS = 8
HEAD_DIM = 64
LEN = 128
D = 512
GROUPS = 16
CHIPS = 32
CORES = 2
ROWS = 320
PIECE = 10
epsilon = 1e-06
f32 = jnp.float32
bf16 = jnp.bfloat16


def nn(a, b):
    return lax.dot_general(a, b, (((1,), (0,)), ((), ())), preferred_element_type=f32)


def nt(a, b):
    return lax.dot_general(a, b, (((1,), (1,)), ((), ())), preferred_element_type=f32)


def tn(a, b):
    return lax.dot_general(a, b, (((0,), (0,)), ((), ())), preferred_element_type=f32)


def sigmoid(x):
    return 0.5 * jnp.tanh(0.5 * x) + 0.5


def store_grads(out_ref, mine_in, mine_out, hgrad_ref, masked):
    for block in range(4):
        grads = nn(mine_in, hgrad_ref[:, block * 512 : (block + 1) * 512]).astype(bf16)
        for j in range(4):
            out_ref[4 * block + j, 0:256, :] = grads[:, j * 128 : (j + 1) * 128]
    grads = nn(mine_out, masked).astype(bf16)
    for block in range(4):
        for p in range(4):
            out_ref[4 * block + p, 256:320, :] = grads[
                p * 64 : (p + 1) * 64, block * 128 : (block + 1) * 128
            ]


def layer_kernel(
    lengths_hbm,
    x_hbm,
    up_hbm,
    win_hbm,
    wout_hbm,
    home_ref,
    send_ref,
    hgrad_ref,
    masked_ref,
    keep_in_ref,
    keep_out_ref,
    act_ref,
    slope_ref,
    wslope_ref,
    weights_ref,
    normed_t,
    gated_t,
    lengths_ref,
    x_ref,
    up_ref,
    win_ref,
    wout_ref,
    arrivals,
):
    parts = [(x_hbm.at[0], x_ref)]
    parts += [(win_hbm.at[:, pl.ds(j * D, D)], win_ref.at[:, pl.ds(j * D, D)]) for j in range(4)]
    parts += [(lengths_hbm, lengths_ref), (wout_hbm, wout_ref), (up_hbm.at[0], up_ref)]
    copies = [
        pltpu.make_async_copy(src, dst, arrivals.at[i]) for i, (src, dst) in enumerate(parts)
    ]
    for copy in copies:
        copy.start()
    position = lax.axis_index("wide")
    core = lax.rem(position, 2)
    copies[0].wait()
    x = x_ref[...].astype(f32)
    inverse = lax.rsqrt(jnp.mean(x * x, axis=-1, keepdims=True) + epsilon)
    unit = x * inverse
    normed = unit.astype(bf16)
    normed_t[...] = unit.astype(bf16).astype(f32).T.reshape(CHIPS, 16, LEN)
    for part in range(4):
        columns = pl.ds(part * D, D)
        copies[1 + part].wait()
        hidden = nn(normed, win_ref[:, columns])
        sig = sigmoid(hidden)
        activated = hidden * sig
        act_ref[:, columns] = activated.astype(bf16)
        slope_ref[:, columns] = sig + activated * (1.0 - sig)

    copies[5].wait()
    length = lengths_ref[position]
    query_at = lax.broadcasted_iota(jnp.int32, (LEN, LEN), 0)
    key_at = lax.broadcasted_iota(jnp.int32, (LEN, LEN), 1)
    allowed = (key_at <= query_at) & (key_at < length)
    first = lax.broadcasted_iota(jnp.int32, (LEN, LEN), 1) < HEAD_DIM

    def by_head(block):
        wide = block.astype(f32)
        return (
            jnp.where(first, wide, 0.0).astype(bf16),
            jnp.where(first, 0.0, wide).astype(bf16),
        )

    attended = []
    for pair in range(HEADS // 2):
        at = pair * 128
        queries = by_head(act_ref[:, 2 * D + at : 2 * D + at + 128])
        keys = act_ref[:, 3 * D + at : 3 * D + at + 128]
        values = by_head(act_ref[:, D + at : D + at + 128])
        for side in range(2):
            scores = nt(queries[side], keys) * HEAD_DIM**-0.5
            sig = sigmoid(scores)
            smooth = scores * sig
            slope = (sig + smooth * (1.0 - sig)) * HEAD_DIM**-0.5
            wslope_ref[2 * pair + side] = jnp.where(allowed, slope, 0.0)
            weights_ref[pair, side * LEN : (side + 1) * LEN, :] = jnp.where(
                allowed, smooth, 0.0
            ).astype(bf16)
        attended.append(
            nn(weights_ref[pair, :LEN, :], values[0]) + nn(weights_ref[pair, LEN:, :], values[1])
        )
    attended = jnp.concatenate(attended, axis=1)
    spread = lax.rsqrt(jnp.mean(attended * attended, axis=-1, keepdims=True) + epsilon)
    unit_attended = attended * spread
    gate = act_ref[:, :D].astype(f32)
    gated = (gate * unit_attended).astype(bf16)
    gated_t[...] = gated.astype(f32).T
    copies[6].wait()
    home_ref[0] = (x + nn(gated, wout_ref[...])).astype(bf16)

    copies[7].wait()
    alive = lax.broadcasted_iota(jnp.int32, (LEN, D), 0) < length
    masked = jnp.where(alive, up_ref[...].astype(f32), 0.0).astype(bf16)
    masked_ref[...] = masked
    gated_grad = nt(masked, wout_ref[...]).astype(bf16).astype(f32)
    hgrad_ref[:, :D] = (
        (gated_grad * unit_attended).astype(bf16).astype(f32) * slope_ref[:, :D]
    ).astype(bf16)
    unit_grad = gated_grad * gate
    overlap = jnp.mean(unit_grad * unit_attended, axis=-1, keepdims=True)
    attended_grad = spread * (unit_grad - unit_attended * overlap)

    for pair in range(HEADS // 2):
        at = pair * 128
        queries = by_head(act_ref[:, 2 * D + at : 2 * D + at + 128])
        keys = by_head(act_ref[:, 3 * D + at : 3 * D + at + 128])
        values = act_ref[:, D + at : D + at + 128]
        grads = by_head(attended_grad[:, at : at + 128])
        both = jnp.concatenate(grads, axis=0)
        weight_grads = nt(both, values)
        value_grad = tn(weights_ref[pair], both)
        score_grads = (
            weight_grads * wslope_ref[2 * pair : 2 * pair + 2].reshape(2 * LEN, LEN)
        ).astype(bf16)
        query_grad = nn(score_grads[:LEN], keys[0]) + nn(score_grads[LEN:], keys[1])
        key_grad = tn(score_grads, jnp.concatenate(queries, axis=0))
        for start, grad in ((D, value_grad), (2 * D, query_grad), (3 * D, key_grad)):
            columns = pl.ds(start + at, 128)
            hgrad_ref[:, columns] = (grad * slope_ref[:, columns]).astype(bf16)

    def mine(side):
        rows = pl.ds(pl.multiple_of(side * 8, 8), 8)
        mine_in = normed_t[:, rows, :].reshape(256, LEN).astype(bf16)
        mine_out = jnp.concatenate(
            [gated_t[pl.ds(side * 8 + i, CHIPS, stride=16), :] for i in range(8)], axis=0
        ).astype(bf16)
        return mine_in, mine_out

    keep_in_ref[...], keep_out_ref[...] = mine(core)
    store_grads(send_ref, *mine(1 - core), hgrad_ref, masked)


def keep_kernel(keep_in_ref, keep_out_ref, hgrad_ref, masked_ref, keep_ref):
    store_grads(keep_ref, keep_in_ref[...], keep_out_ref[...], hgrad_ref, masked_ref[...])


def input_grad_kernel(x_hbm, win_hbm, hgrad_ref, masked_ref, xgrad_ref, x_ref, win_ref, arrivals):
    copies = [
        pltpu.make_async_copy(x_hbm.at[0], x_ref, arrivals.at[0]),
        pltpu.make_async_copy(win_hbm, win_ref, arrivals.at[1]),
    ]
    for copy in copies:
        copy.start()
    copies[0].wait()
    x = x_ref[...].astype(f32)
    inverse = lax.rsqrt(jnp.mean(x * x, axis=-1, keepdims=True) + epsilon)
    unit = x * inverse
    copies[1].wait()
    unit_grad = nt(hgrad_ref[...], win_ref[...])
    overlap = jnp.mean(unit_grad * unit, axis=-1, keepdims=True)
    xgrad_ref[0] = (
        masked_ref[...].astype(f32) + inverse * (unit_grad - unit * overlap)
    ).astype(bf16)


def kept_in(space, *arrays):
    return [pltpu.with_memory_space_constraint(array, space) for array in arrays]


def layer(lengths, x, up, win, wout):
    vmem = pl.BlockSpec(memory_space=pltpu.VMEM)
    hbm = pl.BlockSpec(memory_space=pltpu.HBM)
    shapes = [
        (1, LEN, D),
        (GROUPS, ROWS, 128),
        (LEN, 4 * D),
        (LEN, D),
        (256, LEN),
        (256, LEN),
    ]
    return pl.pallas_call(
        layer_kernel,
        out_shape=[jax.ShapeDtypeStruct(shape, bf16) for shape in shapes],
        in_specs=[hbm] * 5,
        out_specs=[vmem] * 6,
        scratch_shapes=[
            pltpu.VMEM((LEN, 4 * D), bf16),
            pltpu.VMEM((LEN, 4 * D), f32),
            pltpu.VMEM((HEADS, LEN, LEN), f32),
            pltpu.VMEM((HEADS // 2, 2 * LEN, LEN), bf16),
            pltpu.VMEM((CHIPS, 16, LEN), f32),
            pltpu.VMEM((D, LEN), f32),
            pltpu.SMEM((2 * CHIPS,), jnp.int32),
            pltpu.VMEM((LEN, D), bf16),
            pltpu.VMEM((LEN, D), bf16),
            pltpu.VMEM((D, 4 * D), bf16),
            pltpu.VMEM((D, D), bf16),
            pltpu.SemaphoreType.DMA((8,)),
        ],
        compiler_params=pltpu.CompilerParams(vmem_limit_bytes=24 << 20),
        name="layer",
    )(*kept_in(pltpu.HBM, lengths, x, up, win, wout))


def kept_half(keep_in, keep_out, hgrad, masked):
    vmem = pl.BlockSpec(memory_space=pltpu.VMEM)
    return pl.pallas_call(
        keep_kernel,
        out_shape=jax.ShapeDtypeStruct((GROUPS, ROWS, 128), bf16),
        in_specs=[vmem] * 4,
        out_specs=vmem,
        compiler_params=pltpu.CompilerParams(vmem_limit_bytes=8 << 20),
        name="kept_half",
    )(*kept_in(pltpu.VMEM, keep_in, keep_out, hgrad, masked))


def input_gradient(x, win, hgrad, masked):
    vmem = pl.BlockSpec(memory_space=pltpu.VMEM)
    hbm = pl.BlockSpec(memory_space=pltpu.HBM)
    return pl.pallas_call(
        input_grad_kernel,
        out_shape=jax.ShapeDtypeStruct((1, LEN, D), bf16),
        in_specs=[hbm, hbm, vmem, vmem],
        out_specs=vmem,
        scratch_shapes=[
            pltpu.VMEM((LEN, D), bf16),
            pltpu.VMEM((D, 4 * D), bf16),
            pltpu.SemaphoreType.DMA((2,)),
        ],
        compiler_params=pltpu.CompilerParams(vmem_limit_bytes=8 << 20),
        name="input_gradient",
    )(*kept_in(pltpu.HBM, x, win), *kept_in(pltpu.VMEM, hgrad, masked))


def chip_half_kernel(keep_ref, received_ref, out_ref):
    for g in range(GROUPS):
        out_ref[g] = (keep_ref[g].astype(f32) + received_ref[g].astype(f32)).astype(bf16)


def chip_half(keep, received):
    vmem = pl.BlockSpec(memory_space=pltpu.VMEM)
    return pl.pallas_call(
        chip_half_kernel,
        out_shape=jax.ShapeDtypeStruct((GROUPS, ROWS, 128), bf16),
        in_specs=[vmem, vmem],
        out_specs=vmem,
        compiler_params=pltpu.CompilerParams(vmem_limit_bytes=8 << 20),
        name="chip_half",
    )(*kept_in(pltpu.VMEM, keep, received))


def group_sum_kernel(parts_ref, out_ref, total, ordered):
    summed = parts_ref[0].astype(f32)
    for g in range(1, GROUPS):
        summed += parts_ref[g].astype(f32)
    total[...] = summed
    for z in range(CHIPS):
        ordered[PIECE * z : PIECE * z + 8, :] = total[8 * z : 8 * z + 8, :]
        ordered[PIECE * z + 8 : PIECE * z + 10, :] = total[pl.ds(256 + z, 2, stride=CHIPS), :]
    out_ref[...] = ordered[...].astype(bf16)


def group_sum(parts):
    vmem = pl.BlockSpec(memory_space=pltpu.VMEM)
    return pl.pallas_call(
        group_sum_kernel,
        out_shape=jax.ShapeDtypeStruct((CHIPS * PIECE, 128), bf16),
        in_specs=[vmem],
        out_specs=vmem,
        scratch_shapes=[pltpu.VMEM((ROWS, 128), f32), pltpu.VMEM((CHIPS * PIECE, 128), f32)],
        compiler_params=pltpu.CompilerParams(vmem_limit_bytes=8 << 20),
        name="group_sum",
    )(*kept_in(pltpu.VMEM, parts))


def chip_sum_kernel(parts_ref, out_ref, parts, copies):
    parts[...] = parts_ref[...].astype(f32)
    summed = parts[0:PIECE, :]
    for z in range(1, CHIPS):
        summed += parts[PIECE * z : PIECE * (z + 1), :]
    for g in range(GROUPS):
        copies[PIECE * g : PIECE * (g + 1), :] = summed
    out_ref[...] = copies[...].astype(bf16)


def chip_sum(parts):
    vmem = pl.BlockSpec(memory_space=pltpu.VMEM)
    return pl.pallas_call(
        chip_sum_kernel,
        out_shape=jax.ShapeDtypeStruct((GROUPS * PIECE, 128), bf16),
        in_specs=[vmem],
        out_specs=vmem,
        scratch_shapes=[
            pltpu.VMEM((CHIPS * PIECE, 128), f32),
            pltpu.VMEM((GROUPS * PIECE, 128), f32),
        ],
        compiler_params=pltpu.CompilerParams(vmem_limit_bytes=8 << 20),
        name="chip_sum",
    )(*kept_in(pltpu.VMEM, parts))


def finish_kernel(
    scale,
    swap_ref,
    home_ref,
    to_early_ref,
    to_late_ref,
    parts_ref,
    out_ref,
    din_ref,
    dout_ref,
    parts,
):
    position = lax.axis_index("wide")
    chosen = swap_ref[lax.rem(position, CHIPS)] == 1
    late = (position >= CHIPS // 2) & (position < CHIPS * 3 // 2)

    @pl.when(chosen & late)
    def _():
        out_ref[...] = to_late_ref[...]

    @pl.when(chosen & jnp.logical_not(late))
    def _():
        out_ref[...] = to_early_ref[...]

    @pl.when(jnp.logical_not(chosen))
    def _():
        out_ref[...] = home_ref[...]

    parts[...] = parts_ref[...].astype(f32) * scale
    for g in range(GROUPS):
        din_ref[:, g * 128 : (g + 1) * 128] = parts[PIECE * g : PIECE * g + 8, :]
        block, pair = g // 4, g % 4
        dout_ref[2 * pair : 2 * pair + 2, block * 128 : (block + 1) * 128] = parts[
            PIECE * g + 8 : PIECE * g + 10, :
        ]


def finish(scale, swaps, home, to_early, to_late, parts):
    vmem = pl.BlockSpec(memory_space=pltpu.VMEM)
    smem = pl.BlockSpec(memory_space=pltpu.SMEM)
    return pl.pallas_call(
        lambda *refs: finish_kernel(scale, *refs),
        out_shape=(
            jax.ShapeDtypeStruct((1, LEN, D), bf16),
            jax.ShapeDtypeStruct((8, 4 * D), f32),
            jax.ShapeDtypeStruct((8, D), f32),
        ),
        in_specs=[smem, vmem, vmem, vmem, vmem],
        out_specs=(vmem, vmem, vmem),
        scratch_shapes=[pltpu.VMEM((GROUPS * PIECE, 128), f32)],
        compiler_params=pltpu.CompilerParams(vmem_limit_bytes=8 << 20),
        name="finish",
    )(swaps, *kept_in(pltpu.VMEM, home, to_early, to_late, parts))


def exchanged(rows, count, axis, groups=None):
    pieces = rows.reshape(count, PIECE // 2, 2, 128)
    pieces = lax.all_to_all(pieces, axis, 0, 0, tiled=True, axis_index_groups=groups)
    return pieces.reshape(count * PIECE, 128)


def body(sequences, upstream, lengths, swap_table, input_weight, output_weight):
    wide = lax.axis_size("wide")
    half = wide // 2
    home, send, hgrad, masked, keep_in, keep_out = layer(
        lengths.reshape(wide), sequences, upstream, input_weight, output_weight
    )
    late = range(half // 2, half * 3 // 2)
    route = [(i, (i + half) % wide) for i in range(wide)]
    received = lax.ppermute(send, "wide", [(i, i ^ 1) for i in range(wide)])
    keep = kept_half(keep_in, keep_out, hgrad, masked)
    to_early = lax.ppermute(home, "wide", [r for r in route if r[0] in late])
    to_late = lax.ppermute(home, "wide", [r for r in route if r[1] in late])
    chip = chip_half(keep, received)
    parts = lax.all_to_all(chip, "grp", 0, 0, tiled=True)
    input_grad = input_gradient(sequences, input_weight, hgrad, masked)
    parts = group_sum(parts)
    same_core = [[2 * z + c for z in range(CHIPS)] for c in range(CORES)]
    parts = exchanged(parts, CHIPS, "wide", same_core)
    parts = exchanged(chip_sum(parts), GROUPS, "grp")
    scale = 1.0 / math.sqrt(LEN * wide * lax.axis_size("grp"))
    layer_out, total_in, total_out = finish(
        scale, swap_table.reshape(half), home, to_early, to_late, parts
    )
    return (layer_out, input_grad, total_in, total_out)


def solution(mesh):
    placed = (
        P(("grp", "wide"), None, None),
        P(("grp", "wide"), None, None),
        P("grp", None, None),
        P("grp", None, None),
        P(),
        P(),
    )
    return jax.shard_map(
        body,
        mesh=mesh,
        in_specs=placed,
        out_specs=(
            P(("grp", "wide"), None, None),
            P(("grp", "wide"), None, None),
            P("wide", None),
            P("wide", None),
        ),
        check_vma=False,
    )
```

```python
import math

import jax
import jax.numpy as jnp
from jax import lax
from jax.experimental import pallas as pl
from jax.experimental.pallas import tpu as pltpu
from jax.sharding import PartitionSpec as P


HEADS = 8
HEAD_DIM = 64
LEN = 128
D = 512
GROUPS = 16
CHIPS = 32
CORES = 2
ROWS = 320
PIECE = 10
FIRST_CHIP = 19
epsilon = 1e-06
f32 = jnp.float32
bf16 = jnp.bfloat16


def nn(a, b):
    return lax.dot_general(a, b, (((1,), (0,)), ((), ())), preferred_element_type=f32)


def nt(a, b):
    return lax.dot_general(a, b, (((1,), (1,)), ((), ())), preferred_element_type=f32)


def tn(a, b):
    return lax.dot_general(a, b, (((0,), (0,)), ((), ())), preferred_element_type=f32)


def sigmoid(x):
    return 0.5 * jnp.tanh(0.5 * x) + 0.5


def store_grads(out_ref, mine_in, mine_out, hgrad_ref, masked):
    for block in range(4):
        grads = nn(mine_in, hgrad_ref[:, block * 512 : (block + 1) * 512]).astype(bf16)
        for j in range(4):
            out_ref[4 * block + j, 0:256, :] = grads[:, j * 128 : (j + 1) * 128]
    grads = nn(mine_out, masked).astype(bf16)
    for block in range(4):
        for p in range(4):
            out_ref[4 * block + p, 256:320, :] = grads[
                p * 64 : (p + 1) * 64, block * 128 : (block + 1) * 128
            ]


def layer_kernel(
    lengths_hbm,
    x_hbm,
    up_hbm,
    win_hbm,
    wout_hbm,
    home_ref,
    send_ref,
    hgrad_ref,
    masked_ref,
    keep_in_ref,
    keep_out_ref,
    act_ref,
    slope_ref,
    wslope_ref,
    weights_ref,
    normed_t,
    gated_t,
    lengths_ref,
    x_ref,
    up_ref,
    win_ref,
    wout_ref,
    arrivals,
):
    parts = [(x_hbm.at[0], x_ref)]
    parts += [(win_hbm.at[:, pl.ds(j * D, D)], win_ref.at[:, pl.ds(j * D, D)]) for j in range(4)]
    parts += [(lengths_hbm, lengths_ref), (wout_hbm, wout_ref), (up_hbm.at[0], up_ref)]
    copies = [
        pltpu.make_async_copy(src, dst, arrivals.at[i]) for i, (src, dst) in enumerate(parts)
    ]
    for copy in copies:
        copy.start()
    position = lax.axis_index("wide")
    core = lax.rem(position, 2)
    copies[0].wait()
    x = x_ref[...].astype(f32)
    inverse = lax.rsqrt(jnp.mean(x * x, axis=-1, keepdims=True) + epsilon)
    unit = x * inverse
    normed = unit.astype(bf16)
    normed_t[...] = unit.astype(bf16).astype(f32).T.reshape(CHIPS, 16, LEN)
    for part in range(4):
        columns = pl.ds(part * D, D)
        copies[1 + part].wait()
        hidden = nn(normed, win_ref[:, columns])
        sig = sigmoid(hidden)
        activated = hidden * sig
        act_ref[:, columns] = activated.astype(bf16)
        slope_ref[:, columns] = sig + activated * (1.0 - sig)

    copies[5].wait()
    length = lengths_ref[position]
    query_at = lax.broadcasted_iota(jnp.int32, (LEN, LEN), 0)
    key_at = lax.broadcasted_iota(jnp.int32, (LEN, LEN), 1)
    allowed = (key_at <= query_at) & (key_at < length)
    first = lax.broadcasted_iota(jnp.int32, (LEN, LEN), 1) < HEAD_DIM

    def by_head(block):
        wide = block.astype(f32)
        return (
            jnp.where(first, wide, 0.0).astype(bf16),
            jnp.where(first, 0.0, wide).astype(bf16),
        )

    attended = []
    for pair in range(HEADS // 2):
        at = pair * 128
        queries = by_head(act_ref[:, 2 * D + at : 2 * D + at + 128])
        keys = act_ref[:, 3 * D + at : 3 * D + at + 128]
        values = by_head(act_ref[:, D + at : D + at + 128])
        for side in range(2):
            scores = nt(queries[side], keys) * HEAD_DIM**-0.5
            sig = sigmoid(scores)
            smooth = scores * sig
            slope = (sig + smooth * (1.0 - sig)) * HEAD_DIM**-0.5
            wslope_ref[2 * pair + side] = jnp.where(allowed, slope, 0.0)
            weights_ref[pair, side * LEN : (side + 1) * LEN, :] = jnp.where(
                allowed, smooth, 0.0
            ).astype(bf16)
        attended.append(
            nn(weights_ref[pair, :LEN, :], values[0]) + nn(weights_ref[pair, LEN:, :], values[1])
        )
    attended = jnp.concatenate(attended, axis=1)
    spread = lax.rsqrt(jnp.mean(attended * attended, axis=-1, keepdims=True) + epsilon)
    unit_attended = attended * spread
    gate = act_ref[:, :D].astype(f32)
    gated = (gate * unit_attended).astype(bf16)
    gated_t[...] = gated.astype(f32).T
    copies[6].wait()
    home_ref[0] = (x + nn(gated, wout_ref[...])).astype(bf16)

    copies[7].wait()
    alive = lax.broadcasted_iota(jnp.int32, (LEN, D), 0) < length
    masked = jnp.where(alive, up_ref[...].astype(f32), 0.0).astype(bf16)
    masked_ref[...] = masked
    gated_grad = nt(masked, wout_ref[...]).astype(bf16).astype(f32)
    hgrad_ref[:, :D] = (
        (gated_grad * unit_attended).astype(bf16).astype(f32) * slope_ref[:, :D]
    ).astype(bf16)
    unit_grad = gated_grad * gate
    overlap = jnp.mean(unit_grad * unit_attended, axis=-1, keepdims=True)
    attended_grad = spread * (unit_grad - unit_attended * overlap)

    for pair in range(HEADS // 2):
        at = pair * 128
        queries = by_head(act_ref[:, 2 * D + at : 2 * D + at + 128])
        keys = by_head(act_ref[:, 3 * D + at : 3 * D + at + 128])
        values = act_ref[:, D + at : D + at + 128]
        grads = by_head(attended_grad[:, at : at + 128])
        both = jnp.concatenate(grads, axis=0)
        weight_grads = nt(both, values)
        value_grad = tn(weights_ref[pair], both)
        score_grads = (
            weight_grads * wslope_ref[2 * pair : 2 * pair + 2].reshape(2 * LEN, LEN)
        ).astype(bf16)
        query_grad = nn(score_grads[:LEN], keys[0]) + nn(score_grads[LEN:], keys[1])
        key_grad = tn(score_grads, jnp.concatenate(queries, axis=0))
        for start, grad in ((D, value_grad), (2 * D, query_grad), (3 * D, key_grad)):
            columns = pl.ds(start + at, 128)
            hgrad_ref[:, columns] = (grad * slope_ref[:, columns]).astype(bf16)

    def mine(side):
        rows = pl.ds(pl.multiple_of(side * 8, 8), 8)
        mine_in = normed_t[:, rows, :].reshape(256, LEN).astype(bf16)
        mine_out = jnp.concatenate(
            [gated_t[pl.ds(side * 8 + i, CHIPS, stride=16), :] for i in range(8)], axis=0
        ).astype(bf16)
        return mine_in, mine_out

    keep_in_ref[...], keep_out_ref[...] = mine(core)
    store_grads(send_ref, *mine(1 - core), hgrad_ref, masked)


def keep_kernel(keep_in_ref, keep_out_ref, hgrad_ref, masked_ref, keep_ref):
    store_grads(keep_ref, keep_in_ref[...], keep_out_ref[...], hgrad_ref, masked_ref[...])


def input_grad_kernel(x_hbm, win_hbm, hgrad_ref, masked_ref, xgrad_ref, x_ref, win_ref, arrivals):
    copies = [
        pltpu.make_async_copy(x_hbm.at[0], x_ref, arrivals.at[0]),
        pltpu.make_async_copy(win_hbm, win_ref, arrivals.at[1]),
    ]
    for copy in copies:
        copy.start()
    copies[0].wait()
    x = x_ref[...].astype(f32)
    inverse = lax.rsqrt(jnp.mean(x * x, axis=-1, keepdims=True) + epsilon)
    unit = x * inverse
    copies[1].wait()
    unit_grad = nt(hgrad_ref[...], win_ref[...])
    overlap = jnp.mean(unit_grad * unit, axis=-1, keepdims=True)
    xgrad_ref[0] = (
        masked_ref[...].astype(f32) + inverse * (unit_grad - unit * overlap)
    ).astype(bf16)


def kept_in(space, *arrays):
    return [pltpu.with_memory_space_constraint(array, space) for array in arrays]


def layer(lengths, x, up, win, wout):
    vmem = pl.BlockSpec(memory_space=pltpu.VMEM)
    hbm = pl.BlockSpec(memory_space=pltpu.HBM)
    shapes = [
        (1, LEN, D),
        (GROUPS, ROWS, 128),
        (LEN, 4 * D),
        (LEN, D),
        (256, LEN),
        (256, LEN),
    ]
    return pl.pallas_call(
        layer_kernel,
        out_shape=[jax.ShapeDtypeStruct(shape, bf16) for shape in shapes],
        in_specs=[hbm] * 5,
        out_specs=[vmem] * 6,
        scratch_shapes=[
            pltpu.VMEM((LEN, 4 * D), bf16),
            pltpu.VMEM((LEN, 4 * D), f32),
            pltpu.VMEM((HEADS, LEN, LEN), f32),
            pltpu.VMEM((HEADS // 2, 2 * LEN, LEN), bf16),
            pltpu.VMEM((CHIPS, 16, LEN), f32),
            pltpu.VMEM((D, LEN), f32),
            pltpu.SMEM((2 * CHIPS,), jnp.int32),
            pltpu.VMEM((LEN, D), bf16),
            pltpu.VMEM((LEN, D), bf16),
            pltpu.VMEM((D, 4 * D), bf16),
            pltpu.VMEM((D, D), bf16),
            pltpu.SemaphoreType.DMA((8,)),
        ],
        compiler_params=pltpu.CompilerParams(vmem_limit_bytes=24 << 20),
        name="layer",
    )(*kept_in(pltpu.HBM, lengths, x, up, win, wout))


def kept_half(keep_in, keep_out, hgrad, masked):
    vmem = pl.BlockSpec(memory_space=pltpu.VMEM)
    return pl.pallas_call(
        keep_kernel,
        out_shape=jax.ShapeDtypeStruct((GROUPS, ROWS, 128), bf16),
        in_specs=[vmem] * 4,
        out_specs=vmem,
        compiler_params=pltpu.CompilerParams(vmem_limit_bytes=8 << 20),
        name="kept_half",
    )(*kept_in(pltpu.VMEM, keep_in, keep_out, hgrad, masked))


def input_gradient(x, win, hgrad, masked):
    vmem = pl.BlockSpec(memory_space=pltpu.VMEM)
    hbm = pl.BlockSpec(memory_space=pltpu.HBM)
    return pl.pallas_call(
        input_grad_kernel,
        out_shape=jax.ShapeDtypeStruct((1, LEN, D), bf16),
        in_specs=[hbm, hbm, vmem, vmem],
        out_specs=vmem,
        scratch_shapes=[
            pltpu.VMEM((LEN, D), bf16),
            pltpu.VMEM((D, 4 * D), bf16),
            pltpu.SemaphoreType.DMA((2,)),
        ],
        compiler_params=pltpu.CompilerParams(vmem_limit_bytes=8 << 20),
        name="input_gradient",
    )(*kept_in(pltpu.HBM, x, win), *kept_in(pltpu.VMEM, hgrad, masked))


def chip_half_kernel(keep_ref, received_ref, out_ref):
    for g in range(GROUPS):
        out_ref[g] = (keep_ref[g].astype(f32) + received_ref[g].astype(f32)).astype(bf16)


def chip_half(keep, received):
    vmem = pl.BlockSpec(memory_space=pltpu.VMEM)
    return pl.pallas_call(
        chip_half_kernel,
        out_shape=jax.ShapeDtypeStruct((GROUPS, ROWS, 128), bf16),
        in_specs=[vmem, vmem],
        out_specs=vmem,
        compiler_params=pltpu.CompilerParams(vmem_limit_bytes=8 << 20),
        name="chip_half",
    )(*kept_in(pltpu.VMEM, keep, received))


def group_sum_kernel(parts_ref, out_ref, total, ordered):
    summed = parts_ref[0].astype(f32)
    for g in range(1, GROUPS):
        summed += parts_ref[g].astype(f32)
    total[...] = summed
    for j in range(CHIPS):
        z = (FIRST_CHIP + j) % CHIPS
        ordered[PIECE * j : PIECE * j + 8, :] = total[8 * z : 8 * z + 8, :]
        ordered[PIECE * j + 8 : PIECE * j + 10, :] = total[pl.ds(256 + z, 2, stride=CHIPS), :]
    out_ref[...] = ordered[...].astype(bf16)


def group_sum(parts):
    vmem = pl.BlockSpec(memory_space=pltpu.VMEM)
    return pl.pallas_call(
        group_sum_kernel,
        out_shape=jax.ShapeDtypeStruct((CHIPS * PIECE, 128), bf16),
        in_specs=[vmem],
        out_specs=vmem,
        scratch_shapes=[pltpu.VMEM((ROWS, 128), f32), pltpu.VMEM((CHIPS * PIECE, 128), f32)],
        compiler_params=pltpu.CompilerParams(vmem_limit_bytes=8 << 20),
        name="group_sum",
    )(*kept_in(pltpu.VMEM, parts))


def chip_sum_kernel(parts_ref, out_ref, parts, copies):
    parts[...] = parts_ref[...].astype(f32)
    summed = parts[0:PIECE, :]
    for z in range(1, CHIPS):
        summed += parts[PIECE * z : PIECE * (z + 1), :]
    for g in range(GROUPS):
        copies[PIECE * g : PIECE * (g + 1), :] = summed
    out_ref[...] = copies[...].astype(bf16)


def chip_sum(parts):
    vmem = pl.BlockSpec(memory_space=pltpu.VMEM)
    return pl.pallas_call(
        chip_sum_kernel,
        out_shape=jax.ShapeDtypeStruct((GROUPS * PIECE, 128), bf16),
        in_specs=[vmem],
        out_specs=vmem,
        scratch_shapes=[
            pltpu.VMEM((CHIPS * PIECE, 128), f32),
            pltpu.VMEM((GROUPS * PIECE, 128), f32),
        ],
        compiler_params=pltpu.CompilerParams(vmem_limit_bytes=8 << 20),
        name="chip_sum",
    )(*kept_in(pltpu.VMEM, parts))


def finish_kernel(
    scale,
    swap_ref,
    home_ref,
    arrived_ref,
    parts_ref,
    out_ref,
    din_ref,
    dout_ref,
    parts,
):
    position = lax.axis_index("wide")
    chosen = swap_ref[lax.rem(position, CHIPS)] == 1

    @pl.when(chosen)
    def _():
        out_ref[...] = arrived_ref[...]

    @pl.when(jnp.logical_not(chosen))
    def _():
        out_ref[...] = home_ref[...]

    parts[...] = parts_ref[...].astype(f32) * scale
    for g in range(GROUPS):
        din_ref[:, g * 128 : (g + 1) * 128] = parts[PIECE * g : PIECE * g + 8, :]
        block, pair = g // 4, g % 4
        dout_ref[2 * pair : 2 * pair + 2, block * 128 : (block + 1) * 128] = parts[
            PIECE * g + 8 : PIECE * g + 10, :
        ]


def finish(scale, swaps, home, arrived, parts):
    vmem = pl.BlockSpec(memory_space=pltpu.VMEM)
    smem = pl.BlockSpec(memory_space=pltpu.SMEM)
    return pl.pallas_call(
        lambda *refs: finish_kernel(scale, *refs),
        out_shape=(
            jax.ShapeDtypeStruct((1, LEN, D), bf16),
            jax.ShapeDtypeStruct((8, 4 * D), f32),
            jax.ShapeDtypeStruct((8, D), f32),
        ),
        in_specs=[smem, vmem, vmem, vmem],
        out_specs=(vmem, vmem, vmem),
        scratch_shapes=[pltpu.VMEM((GROUPS * PIECE, 128), f32)],
        compiler_params=pltpu.CompilerParams(vmem_limit_bytes=8 << 20),
        name="finish",
    )(swaps, *kept_in(pltpu.VMEM, home, arrived, parts))


def exchanged(rows, count, axis, groups=None):
    pieces = rows.reshape(count, PIECE // 2, 2, 128)
    pieces = lax.all_to_all(pieces, axis, 0, 0, tiled=True, axis_index_groups=groups)
    return pieces.reshape(count * PIECE, 128)


def body(sequences, upstream, lengths, swap_table, input_weight, output_weight):
    wide = lax.axis_size("wide")
    half = wide // 2
    home, send, hgrad, masked, keep_in, keep_out = layer(
        lengths.reshape(wide), sequences, upstream, input_weight, output_weight
    )
    same_core = [
        [2 * ((FIRST_CHIP + j) % CHIPS) + c for j in range(CHIPS)] for c in range(CORES)
    ]
    received = lax.ppermute(send, "wide", [(i, i ^ 1) for i in range(wide)])
    keep = kept_half(keep_in, keep_out, hgrad, masked)
    arrived = lax.ppermute(home, "wide", [(i, (i + half) % wide) for i in range(wide)])
    chip = chip_half(keep, received)
    parts = lax.all_to_all(chip, "grp", 0, 0, tiled=True)
    input_grad = input_gradient(sequences, input_weight, hgrad, masked)
    parts = group_sum(parts)
    parts = exchanged(parts, CHIPS, "wide", same_core)
    parts = chip_sum(parts)
    parts = exchanged(parts, GROUPS, "grp")
    scale = 1.0 / math.sqrt(LEN * wide * lax.axis_size("grp"))
    layer_out, total_in, total_out = finish(
        scale, swap_table.reshape(half), home, arrived, parts
    )
    return (layer_out, input_grad, total_in, total_out)


def solution(mesh):
    placed = (
        P(("grp", "wide"), None, None),
        P(("grp", "wide"), None, None),
        P("grp", None, None),
        P("grp", None, None),
        P(),
        P(),
    )
    return jax.shard_map(
        body,
        mesh=mesh,
        in_specs=placed,
        out_specs=(
            P(("grp", "wide"), None, None),
            P(("grp", "wide"), None, None),
            P("wide", None),
            P("wide", None),
        ),
        check_vma=False,
    )
```

```python
import math

import jax
import jax.numpy as jnp
from jax import lax
from jax.experimental import pallas as pl
from jax.experimental.pallas import tpu as pltpu
from jax.sharding import PartitionSpec as P


HEADS = 8
HEAD_DIM = 64
LEN = 128
D = 512
GROUPS = 16
CHIPS = 32
CORES = 2
ROWS = 320
PIECE = 10
FIRST_CHIP = 22
FIRST_GROUP = 10
epsilon = 1e-06
f32 = jnp.float32
bf16 = jnp.bfloat16


def nn(a, b):
    return lax.dot_general(a, b, (((1,), (0,)), ((), ())), preferred_element_type=f32)


def nt(a, b):
    return lax.dot_general(a, b, (((1,), (1,)), ((), ())), preferred_element_type=f32)


def tn(a, b):
    return lax.dot_general(a, b, (((0,), (0,)), ((), ())), preferred_element_type=f32)


def sigmoid(x):
    return 0.5 * jnp.tanh(0.5 * x) + 0.5


def place(group):
    return (group - FIRST_GROUP) % GROUPS


def store_grads(out_ref, mine_in, mine_out, hgrad_ref, masked):
    for block in range(4):
        grads = nn(mine_in, hgrad_ref[:, block * 512 : (block + 1) * 512]).astype(bf16)
        for j in range(4):
            out_ref[place(4 * block + j), 0:256, :] = grads[:, j * 128 : (j + 1) * 128]
    grads = nn(mine_out, masked).astype(bf16)
    for block in range(4):
        for p in range(4):
            out_ref[place(4 * block + p), 256:320, :] = grads[
                p * 64 : (p + 1) * 64, block * 128 : (block + 1) * 128
            ]


def layer_kernel(
    lengths_hbm,
    x_hbm,
    up_hbm,
    win_hbm,
    wout_hbm,
    home_ref,
    send_ref,
    hgrad_ref,
    masked_ref,
    keep_in_ref,
    keep_out_ref,
    act_ref,
    slope_ref,
    wslope_ref,
    weights_ref,
    normed_t,
    gated_t,
    lengths_ref,
    x_ref,
    up_ref,
    win_ref,
    wout_ref,
    arrivals,
):
    parts = [(x_hbm.at[0], x_ref)]
    parts += [(win_hbm.at[:, pl.ds(j * D, D)], win_ref.at[:, pl.ds(j * D, D)]) for j in range(4)]
    parts += [(lengths_hbm, lengths_ref), (wout_hbm, wout_ref), (up_hbm.at[0], up_ref)]
    copies = [
        pltpu.make_async_copy(src, dst, arrivals.at[i]) for i, (src, dst) in enumerate(parts)
    ]
    for copy in copies:
        copy.start()
    position = lax.axis_index("wide")
    core = lax.rem(position, 2)
    copies[0].wait()
    x = x_ref[...].astype(f32)
    inverse = lax.rsqrt(jnp.mean(x * x, axis=-1, keepdims=True) + epsilon)
    unit = x * inverse
    normed = unit.astype(bf16)
    normed_t[...] = unit.astype(bf16).astype(f32).T.reshape(CHIPS, 16, LEN)
    for part in range(4):
        columns = pl.ds(part * D, D)
        copies[1 + part].wait()
        hidden = nn(normed, win_ref[:, columns])
        sig = sigmoid(hidden)
        activated = hidden * sig
        act_ref[:, columns] = activated.astype(bf16)
        slope_ref[:, columns] = sig + activated * (1.0 - sig)

    copies[5].wait()
    length = lengths_ref[position]
    query_at = lax.broadcasted_iota(jnp.int32, (LEN, LEN), 0)
    key_at = lax.broadcasted_iota(jnp.int32, (LEN, LEN), 1)
    allowed = (key_at <= query_at) & (key_at < length)
    first = lax.broadcasted_iota(jnp.int32, (LEN, LEN), 1) < HEAD_DIM

    def by_head(block):
        wide = block.astype(f32)
        return (
            jnp.where(first, wide, 0.0).astype(bf16),
            jnp.where(first, 0.0, wide).astype(bf16),
        )

    attended = []
    for pair in range(HEADS // 2):
        at = pair * 128
        queries = by_head(act_ref[:, 2 * D + at : 2 * D + at + 128])
        keys = act_ref[:, 3 * D + at : 3 * D + at + 128]
        values = by_head(act_ref[:, D + at : D + at + 128])
        for side in range(2):
            scores = nt(queries[side], keys) * HEAD_DIM**-0.5
            sig = sigmoid(scores)
            smooth = scores * sig
            slope = (sig + smooth * (1.0 - sig)) * HEAD_DIM**-0.5
            wslope_ref[2 * pair + side] = jnp.where(allowed, slope, 0.0)
            weights_ref[pair, side * LEN : (side + 1) * LEN, :] = jnp.where(
                allowed, smooth, 0.0
            ).astype(bf16)
        attended.append(
            nn(weights_ref[pair, :LEN, :], values[0]) + nn(weights_ref[pair, LEN:, :], values[1])
        )
    attended = jnp.concatenate(attended, axis=1)
    spread = lax.rsqrt(jnp.mean(attended * attended, axis=-1, keepdims=True) + epsilon)
    unit_attended = attended * spread
    gate = act_ref[:, :D].astype(f32)
    gated = (gate * unit_attended).astype(bf16)
    gated_t[...] = gated.astype(f32).T
    copies[6].wait()
    home_ref[0] = (x + nn(gated, wout_ref[...])).astype(bf16)

    copies[7].wait()
    alive = lax.broadcasted_iota(jnp.int32, (LEN, D), 0) < length
    masked = jnp.where(alive, up_ref[...].astype(f32), 0.0).astype(bf16)
    masked_ref[...] = masked
    gated_grad = nt(masked, wout_ref[...]).astype(bf16).astype(f32)
    hgrad_ref[:, :D] = (
        (gated_grad * unit_attended).astype(bf16).astype(f32) * slope_ref[:, :D]
    ).astype(bf16)
    unit_grad = gated_grad * gate
    overlap = jnp.mean(unit_grad * unit_attended, axis=-1, keepdims=True)
    attended_grad = spread * (unit_grad - unit_attended * overlap)

    for pair in range(HEADS // 2):
        at = pair * 128
        queries = by_head(act_ref[:, 2 * D + at : 2 * D + at + 128])
        keys = by_head(act_ref[:, 3 * D + at : 3 * D + at + 128])
        values = act_ref[:, D + at : D + at + 128]
        grads = by_head(attended_grad[:, at : at + 128])
        both = jnp.concatenate(grads, axis=0)
        weight_grads = nt(both, values)
        value_grad = tn(weights_ref[pair], both)
        score_grads = (
            weight_grads * wslope_ref[2 * pair : 2 * pair + 2].reshape(2 * LEN, LEN)
        ).astype(bf16)
        query_grad = nn(score_grads[:LEN], keys[0]) + nn(score_grads[LEN:], keys[1])
        key_grad = tn(score_grads, jnp.concatenate(queries, axis=0))
        for start, grad in ((D, value_grad), (2 * D, query_grad), (3 * D, key_grad)):
            columns = pl.ds(start + at, 128)
            hgrad_ref[:, columns] = (grad * slope_ref[:, columns]).astype(bf16)

    def mine(side):
        rows = pl.ds(pl.multiple_of(side * 8, 8), 8)
        mine_in = normed_t[:, rows, :].reshape(256, LEN).astype(bf16)
        mine_out = jnp.concatenate(
            [gated_t[pl.ds(side * 8 + i, CHIPS, stride=16), :] for i in range(8)], axis=0
        ).astype(bf16)
        return mine_in, mine_out

    keep_in_ref[...], keep_out_ref[...] = mine(core)
    store_grads(send_ref, *mine(1 - core), hgrad_ref, masked)


def keep_kernel(keep_in_ref, keep_out_ref, hgrad_ref, masked_ref, keep_ref):
    store_grads(keep_ref, keep_in_ref[...], keep_out_ref[...], hgrad_ref, masked_ref[...])


def input_grad_kernel(x_hbm, win_hbm, hgrad_ref, masked_ref, xgrad_ref, x_ref, win_ref, arrivals):
    copies = [
        pltpu.make_async_copy(x_hbm.at[0], x_ref, arrivals.at[0]),
        pltpu.make_async_copy(win_hbm, win_ref, arrivals.at[1]),
    ]
    for copy in copies:
        copy.start()
    copies[0].wait()
    x = x_ref[...].astype(f32)
    inverse = lax.rsqrt(jnp.mean(x * x, axis=-1, keepdims=True) + epsilon)
    unit = x * inverse
    copies[1].wait()
    unit_grad = nt(hgrad_ref[...], win_ref[...])
    overlap = jnp.mean(unit_grad * unit, axis=-1, keepdims=True)
    xgrad_ref[0] = (
        masked_ref[...].astype(f32) + inverse * (unit_grad - unit * overlap)
    ).astype(bf16)


def kept_in(space, *arrays):
    return [pltpu.with_memory_space_constraint(array, space) for array in arrays]


def layer(lengths, x, up, win, wout):
    vmem = pl.BlockSpec(memory_space=pltpu.VMEM)
    hbm = pl.BlockSpec(memory_space=pltpu.HBM)
    shapes = [
        (1, LEN, D),
        (GROUPS, ROWS, 128),
        (LEN, 4 * D),
        (LEN, D),
        (256, LEN),
        (256, LEN),
    ]
    return pl.pallas_call(
        layer_kernel,
        out_shape=[jax.ShapeDtypeStruct(shape, bf16) for shape in shapes],
        in_specs=[hbm] * 5,
        out_specs=[vmem] * 6,
        scratch_shapes=[
            pltpu.VMEM((LEN, 4 * D), bf16),
            pltpu.VMEM((LEN, 4 * D), f32),
            pltpu.VMEM((HEADS, LEN, LEN), f32),
            pltpu.VMEM((HEADS // 2, 2 * LEN, LEN), bf16),
            pltpu.VMEM((CHIPS, 16, LEN), f32),
            pltpu.VMEM((D, LEN), f32),
            pltpu.SMEM((2 * CHIPS,), jnp.int32),
            pltpu.VMEM((LEN, D), bf16),
            pltpu.VMEM((LEN, D), bf16),
            pltpu.VMEM((D, 4 * D), bf16),
            pltpu.VMEM((D, D), bf16),
            pltpu.SemaphoreType.DMA((8,)),
        ],
        compiler_params=pltpu.CompilerParams(vmem_limit_bytes=24 << 20),
        name="layer",
    )(*kept_in(pltpu.HBM, lengths, x, up, win, wout))


def kept_half(keep_in, keep_out, hgrad, masked):
    vmem = pl.BlockSpec(memory_space=pltpu.VMEM)
    return pl.pallas_call(
        keep_kernel,
        out_shape=jax.ShapeDtypeStruct((GROUPS, ROWS, 128), bf16),
        in_specs=[vmem] * 4,
        out_specs=vmem,
        compiler_params=pltpu.CompilerParams(vmem_limit_bytes=8 << 20),
        name="kept_half",
    )(*kept_in(pltpu.VMEM, keep_in, keep_out, hgrad, masked))


def input_gradient(x, win, hgrad, masked):
    vmem = pl.BlockSpec(memory_space=pltpu.VMEM)
    hbm = pl.BlockSpec(memory_space=pltpu.HBM)
    return pl.pallas_call(
        input_grad_kernel,
        out_shape=jax.ShapeDtypeStruct((1, LEN, D), bf16),
        in_specs=[hbm, hbm, vmem, vmem],
        out_specs=vmem,
        scratch_shapes=[
            pltpu.VMEM((LEN, D), bf16),
            pltpu.VMEM((D, 4 * D), bf16),
            pltpu.SemaphoreType.DMA((2,)),
        ],
        compiler_params=pltpu.CompilerParams(vmem_limit_bytes=8 << 20),
        name="input_gradient",
    )(*kept_in(pltpu.HBM, x, win), *kept_in(pltpu.VMEM, hgrad, masked))


def chip_half_kernel(keep_ref, received_ref, out_ref):
    for g in range(GROUPS):
        out_ref[g] = (keep_ref[g].astype(f32) + received_ref[g].astype(f32)).astype(bf16)


def chip_half(keep, received):
    vmem = pl.BlockSpec(memory_space=pltpu.VMEM)
    return pl.pallas_call(
        chip_half_kernel,
        out_shape=jax.ShapeDtypeStruct((GROUPS, ROWS, 128), bf16),
        in_specs=[vmem, vmem],
        out_specs=vmem,
        compiler_params=pltpu.CompilerParams(vmem_limit_bytes=8 << 20),
        name="chip_half",
    )(*kept_in(pltpu.VMEM, keep, received))


def group_sum_kernel(parts_ref, out_ref, total, ordered):
    summed = parts_ref[0].astype(f32)
    for g in range(1, GROUPS):
        summed += parts_ref[g].astype(f32)
    total[...] = summed
    for j in range(CHIPS):
        z = (FIRST_CHIP + j) % CHIPS
        ordered[PIECE * j : PIECE * j + 8, :] = total[8 * z : 8 * z + 8, :]
        ordered[PIECE * j + 8 : PIECE * j + 10, :] = total[pl.ds(256 + z, 2, stride=CHIPS), :]
    out_ref[...] = ordered[...].astype(bf16)


def group_sum(parts):
    vmem = pl.BlockSpec(memory_space=pltpu.VMEM)
    return pl.pallas_call(
        group_sum_kernel,
        out_shape=jax.ShapeDtypeStruct((CHIPS * PIECE, 128), bf16),
        in_specs=[vmem],
        out_specs=vmem,
        scratch_shapes=[pltpu.VMEM((ROWS, 128), f32), pltpu.VMEM((CHIPS * PIECE, 128), f32)],
        compiler_params=pltpu.CompilerParams(vmem_limit_bytes=8 << 20),
        name="group_sum",
    )(*kept_in(pltpu.VMEM, parts))


def chip_sum_kernel(parts_ref, out_ref, parts, copies):
    parts[...] = parts_ref[...].astype(f32)
    summed = parts[0:PIECE, :]
    for z in range(1, CHIPS):
        summed += parts[PIECE * z : PIECE * (z + 1), :]
    for g in range(GROUPS):
        copies[PIECE * g : PIECE * (g + 1), :] = summed
    out_ref[...] = copies[...].astype(bf16)


def chip_sum(parts):
    vmem = pl.BlockSpec(memory_space=pltpu.VMEM)
    return pl.pallas_call(
        chip_sum_kernel,
        out_shape=jax.ShapeDtypeStruct((GROUPS * PIECE, 128), bf16),
        in_specs=[vmem],
        out_specs=vmem,
        scratch_shapes=[
            pltpu.VMEM((CHIPS * PIECE, 128), f32),
            pltpu.VMEM((GROUPS * PIECE, 128), f32),
        ],
        compiler_params=pltpu.CompilerParams(vmem_limit_bytes=8 << 20),
        name="chip_sum",
    )(*kept_in(pltpu.VMEM, parts))


def finish_kernel(
    scale,
    swap_ref,
    home_ref,
    arrived_ref,
    parts_ref,
    out_ref,
    din_ref,
    dout_ref,
    parts,
):
    position = lax.axis_index("wide")
    chosen = swap_ref[lax.rem(position, CHIPS)] == 1

    @pl.when(chosen)
    def _():
        out_ref[...] = arrived_ref[...]

    @pl.when(jnp.logical_not(chosen))
    def _():
        out_ref[...] = home_ref[...]

    parts[...] = parts_ref[...].astype(f32) * scale
    for g in range(GROUPS):
        din_ref[:, g * 128 : (g + 1) * 128] = parts[PIECE * g : PIECE * g + 8, :]
        block, pair = g // 4, g % 4
        dout_ref[2 * pair : 2 * pair + 2, block * 128 : (block + 1) * 128] = parts[
            PIECE * g + 8 : PIECE * g + 10, :
        ]


def finish(scale, swaps, home, arrived, parts):
    vmem = pl.BlockSpec(memory_space=pltpu.VMEM)
    smem = pl.BlockSpec(memory_space=pltpu.SMEM)
    return pl.pallas_call(
        lambda *refs: finish_kernel(scale, *refs),
        out_shape=(
            jax.ShapeDtypeStruct((1, LEN, D), bf16),
            jax.ShapeDtypeStruct((8, 4 * D), f32),
            jax.ShapeDtypeStruct((8, D), f32),
        ),
        in_specs=[smem, vmem, vmem, vmem],
        out_specs=(vmem, vmem, vmem),
        scratch_shapes=[pltpu.VMEM((GROUPS * PIECE, 128), f32)],
        compiler_params=pltpu.CompilerParams(vmem_limit_bytes=8 << 20),
        name="finish",
    )(swaps, *kept_in(pltpu.VMEM, home, arrived, parts))


def exchanged(rows, count, axis, groups=None):
    pieces = rows.reshape(count, PIECE // 2, 2, 128)
    pieces = lax.all_to_all(pieces, axis, 0, 0, tiled=True, axis_index_groups=groups)
    return pieces.reshape(count * PIECE, 128)


def body(sequences, upstream, lengths, swap_table, input_weight, output_weight):
    wide = lax.axis_size("wide")
    half = wide // 2
    home, send, hgrad, masked, keep_in, keep_out = layer(
        lengths.reshape(wide), sequences, upstream, input_weight, output_weight
    )
    plane = [[(FIRST_GROUP + j) % GROUPS for j in range(GROUPS)]]
    same_core = [
        [2 * ((FIRST_CHIP + j) % CHIPS) + c for j in range(CHIPS)] for c in range(CORES)
    ]
    received = lax.ppermute(send, "wide", [(i, i ^ 1) for i in range(wide)])
    keep = kept_half(keep_in, keep_out, hgrad, masked)
    arrived = lax.ppermute(home, "wide", [(i, (i + half) % wide) for i in range(wide)])
    chip = chip_half(keep, received)
    parts = lax.all_to_all(chip, "grp", 0, 0, tiled=True, axis_index_groups=plane)
    input_grad = input_gradient(sequences, input_weight, hgrad, masked)
    parts = group_sum(parts)
    parts = exchanged(parts, CHIPS, "wide", same_core)
    parts = chip_sum(parts)
    parts = exchanged(parts, GROUPS, "grp")
    scale = 1.0 / math.sqrt(LEN * wide * lax.axis_size("grp"))
    layer_out, total_in, total_out = finish(
        scale, swap_table.reshape(half), home, arrived, parts
    )
    return (layer_out, input_grad, total_in, total_out)


def solution(mesh):
    placed = (
        P(("grp", "wide"), None, None),
        P(("grp", "wide"), None, None),
        P("grp", None, None),
        P("grp", None, None),
        P(),
        P(),
    )
    return jax.shard_map(
        body,
        mesh=mesh,
        in_specs=placed,
        out_specs=(
            P(("grp", "wide"), None, None),
            P(("grp", "wide"), None, None),
            P("wide", None),
            P("wide", None),
        ),
        check_vma=False,
    )
```

```python
import math

import jax
import jax.numpy as jnp
from jax import lax
from jax.experimental import pallas as pl
from jax.experimental.pallas import tpu as pltpu
from jax.sharding import PartitionSpec as P


HEADS = 8
HEAD_DIM = 64
LEN = 128
D = 512
GROUPS = 16
CHIPS = 32
CORES = 2
ROWS = 320
PIECE = 10
FIRST_CHIP = 22
FIRST_GROUP = 10
epsilon = 1e-06
f32 = jnp.float32
bf16 = jnp.bfloat16


def nn(a, b):
    return lax.dot_general(a, b, (((1,), (0,)), ((), ())), preferred_element_type=f32)


def nt(a, b):
    return lax.dot_general(a, b, (((1,), (1,)), ((), ())), preferred_element_type=f32)


def tn(a, b):
    return lax.dot_general(a, b, (((0,), (0,)), ((), ())), preferred_element_type=f32)


def sigmoid(x):
    return 0.5 * jnp.tanh(0.5 * x) + 0.5


def place(group):
    return (group - FIRST_GROUP) % GROUPS


def layer_kernel(
    lengths_hbm,
    x_hbm,
    up_hbm,
    win_hbm,
    wout_hbm,
    home_ref,
    factors_ref,
    mine_ref,
    act_ref,
    slope_ref,
    wslope_ref,
    weights_ref,
    normed_t,
    gated_t,
    lengths_ref,
    x_ref,
    up_ref,
    win_ref,
    wout_ref,
    arrivals,
):
    parts = [(x_hbm.at[0], x_ref)]
    parts += [(win_hbm.at[:, pl.ds(j * D, D)], win_ref.at[:, pl.ds(j * D, D)]) for j in range(4)]
    parts += [(lengths_hbm, lengths_ref), (wout_hbm, wout_ref), (up_hbm.at[0], up_ref)]
    copies = [
        pltpu.make_async_copy(src, dst, arrivals.at[i]) for i, (src, dst) in enumerate(parts)
    ]
    for copy in copies:
        copy.start()
    position = lax.axis_index("wide")
    core = lax.rem(position, 2)
    copies[0].wait()
    x = x_ref[...].astype(f32)
    inverse = lax.rsqrt(jnp.mean(x * x, axis=-1, keepdims=True) + epsilon)
    unit = x * inverse
    normed = unit.astype(bf16)
    normed_t[...] = unit.astype(bf16).astype(f32).T.reshape(CHIPS, 16, LEN)
    for part in range(4):
        columns = pl.ds(part * D, D)
        copies[1 + part].wait()
        hidden = nn(normed, win_ref[:, columns])
        sig = sigmoid(hidden)
        activated = hidden * sig
        act_ref[:, columns] = activated.astype(bf16)
        slope_ref[:, columns] = sig + activated * (1.0 - sig)

    copies[5].wait()
    length = lengths_ref[position]
    query_at = lax.broadcasted_iota(jnp.int32, (LEN, LEN), 0)
    key_at = lax.broadcasted_iota(jnp.int32, (LEN, LEN), 1)
    allowed = (key_at <= query_at) & (key_at < length)
    first = lax.broadcasted_iota(jnp.int32, (LEN, LEN), 1) < HEAD_DIM

    def by_head(block):
        wide = block.astype(f32)
        return (
            jnp.where(first, wide, 0.0).astype(bf16),
            jnp.where(first, 0.0, wide).astype(bf16),
        )

    attended = []
    for pair in range(HEADS // 2):
        at = pair * 128
        queries = by_head(act_ref[:, 2 * D + at : 2 * D + at + 128])
        keys = act_ref[:, 3 * D + at : 3 * D + at + 128]
        values = by_head(act_ref[:, D + at : D + at + 128])
        for side in range(2):
            scores = nt(queries[side], keys) * HEAD_DIM**-0.5
            sig = sigmoid(scores)
            smooth = scores * sig
            slope = (sig + smooth * (1.0 - sig)) * HEAD_DIM**-0.5
            wslope_ref[2 * pair + side] = jnp.where(allowed, slope, 0.0)
            weights_ref[pair, side * LEN : (side + 1) * LEN, :] = jnp.where(
                allowed, smooth, 0.0
            ).astype(bf16)
        attended.append(
            nn(weights_ref[pair, :LEN, :], values[0]) + nn(weights_ref[pair, LEN:, :], values[1])
        )
    attended = jnp.concatenate(attended, axis=1)
    spread = lax.rsqrt(jnp.mean(attended * attended, axis=-1, keepdims=True) + epsilon)
    unit_attended = attended * spread
    gate = act_ref[:, :D].astype(f32)
    gated = (gate * unit_attended).astype(bf16)
    gated_t[...] = gated.astype(f32).T
    copies[6].wait()
    home_ref[0] = (x + nn(gated, wout_ref[...])).astype(bf16)

    copies[7].wait()
    alive = lax.broadcasted_iota(jnp.int32, (LEN, D), 0) < length
    masked = jnp.where(alive, up_ref[...].astype(f32), 0.0).astype(bf16)
    factors_ref[:, 4 * D : 5 * D] = masked
    gated_grad = nt(masked, wout_ref[...]).astype(bf16).astype(f32)
    factors_ref[:, :D] = (
        (gated_grad * unit_attended).astype(bf16).astype(f32) * slope_ref[:, :D]
    ).astype(bf16)
    unit_grad = gated_grad * gate
    overlap = jnp.mean(unit_grad * unit_attended, axis=-1, keepdims=True)
    attended_grad = spread * (unit_grad - unit_attended * overlap)

    for pair in range(HEADS // 2):
        at = pair * 128
        queries = by_head(act_ref[:, 2 * D + at : 2 * D + at + 128])
        keys = by_head(act_ref[:, 3 * D + at : 3 * D + at + 128])
        values = act_ref[:, D + at : D + at + 128]
        grads = by_head(attended_grad[:, at : at + 128])
        both = jnp.concatenate(grads, axis=0)
        weight_grads = nt(both, values)
        value_grad = tn(weights_ref[pair], both)
        score_grads = (
            weight_grads * wslope_ref[2 * pair : 2 * pair + 2].reshape(2 * LEN, LEN)
        ).astype(bf16)
        query_grad = nn(score_grads[:LEN], keys[0]) + nn(score_grads[LEN:], keys[1])
        key_grad = tn(score_grads, jnp.concatenate(queries, axis=0))
        for start, grad in ((D, value_grad), (2 * D, query_grad), (3 * D, key_grad)):
            columns = pl.ds(start + at, 128)
            factors_ref[:, columns] = (grad * slope_ref[:, columns]).astype(bf16)

    def columns_of(side):
        rows = pl.ds(pl.multiple_of(side * 8, 8), 8)
        normed_part = normed_t[:, rows, :].reshape(256, LEN).astype(bf16)
        gated_part = jnp.concatenate(
            [gated_t[pl.ds(side * 8 + i, CHIPS, stride=16), :] for i in range(8)], axis=0
        ).astype(bf16)
        return (normed_part[:128], normed_part[128:], gated_part[:128], gated_part[128:])

    for i, block in enumerate(columns_of(1 - core)):
        factors_ref[:, 5 * D + 128 * i : 5 * D + 128 * (i + 1)] = block
    for i, block in enumerate(columns_of(core)):
        mine_ref[128 * i : 128 * (i + 1), :] = block


def pair_kernel(factors_ref, received_ref, mine_ref, out_hbm, out_ref, sent):
    theirs = [received_ref[:, 5 * D + 128 * i : 5 * D + 128 * (i + 1)] for i in range(4)]
    theirs = jnp.concatenate(theirs, axis=0)
    left = jnp.concatenate([mine_ref[...], theirs], axis=1)

    def right(start, width):
        columns = pl.ds(start, width)
        return jnp.concatenate([factors_ref[:, columns], received_ref[:, columns]], axis=0)

    grads_out = nn(left[256:], right(4 * D, D)).astype(bf16)
    copies = []
    for block in range(4):
        grads = nn(left[:256], right(block * D, D)).astype(bf16)
        for j in range(4):
            at = place(4 * block + j)
            out_ref[at, 0:256, :] = grads[:, j * 128 : (j + 1) * 128]
            out_ref[at, 256:320, :] = grads_out[
                j * 64 : (j + 1) * 64, block * 128 : (block + 1) * 128
            ]
            copies.append(
                pltpu.make_async_copy(out_ref.at[at], out_hbm.at[at], sent.at[4 * block + j])
            )
            copies[-1].start()
    for copy in copies:
        copy.wait()


def input_grad_kernel(x_hbm, win_hbm, factors_ref, xgrad_ref, x_ref, win_ref, arrivals):
    copies = [
        pltpu.make_async_copy(x_hbm.at[0], x_ref, arrivals.at[0]),
        pltpu.make_async_copy(win_hbm, win_ref, arrivals.at[1]),
    ]
    for copy in copies:
        copy.start()
    copies[0].wait()
    x = x_ref[...].astype(f32)
    inverse = lax.rsqrt(jnp.mean(x * x, axis=-1, keepdims=True) + epsilon)
    unit = x * inverse
    copies[1].wait()
    unit_grad = nt(factors_ref[:, : 4 * D], win_ref[...])
    overlap = jnp.mean(unit_grad * unit, axis=-1, keepdims=True)
    xgrad_ref[0] = (
        factors_ref[:, 4 * D : 5 * D].astype(f32) + inverse * (unit_grad - unit * overlap)
    ).astype(bf16)


def kept_in(space, *arrays):
    return [pltpu.with_memory_space_constraint(array, space) for array in arrays]


def layer(lengths, x, up, win, wout):
    vmem = pl.BlockSpec(memory_space=pltpu.VMEM)
    hbm = pl.BlockSpec(memory_space=pltpu.HBM)
    shapes = [(1, LEN, D), (LEN, 6 * D), (512, LEN)]
    return pl.pallas_call(
        layer_kernel,
        out_shape=[jax.ShapeDtypeStruct(shape, bf16) for shape in shapes],
        in_specs=[hbm] * 5,
        out_specs=[vmem] * 3,
        scratch_shapes=[
            pltpu.VMEM((LEN, 4 * D), bf16),
            pltpu.VMEM((LEN, 4 * D), f32),
            pltpu.VMEM((HEADS, LEN, LEN), f32),
            pltpu.VMEM((HEADS // 2, 2 * LEN, LEN), bf16),
            pltpu.VMEM((CHIPS, 16, LEN), f32),
            pltpu.VMEM((D, LEN), f32),
            pltpu.SMEM((2 * CHIPS,), jnp.int32),
            pltpu.VMEM((LEN, D), bf16),
            pltpu.VMEM((LEN, D), bf16),
            pltpu.VMEM((D, 4 * D), bf16),
            pltpu.VMEM((D, D), bf16),
            pltpu.SemaphoreType.DMA((8,)),
        ],
        compiler_params=pltpu.CompilerParams(vmem_limit_bytes=24 << 20),
        name="layer",
    )(*kept_in(pltpu.HBM, lengths, x, up, win, wout))


def pair_half(factors, received, mine):
    vmem = pl.BlockSpec(memory_space=pltpu.VMEM)
    shape = (GROUPS, ROWS, 128)
    return pl.pallas_call(
        pair_kernel,
        out_shape=jax.ShapeDtypeStruct(shape, bf16),
        in_specs=[vmem] * 3,
        out_specs=pl.BlockSpec(memory_space=pltpu.HBM),
        scratch_shapes=[pltpu.VMEM(shape, bf16), pltpu.SemaphoreType.DMA((GROUPS,))],
        compiler_params=pltpu.CompilerParams(vmem_limit_bytes=12 << 20),
        name="pair_half",
    )(*kept_in(pltpu.VMEM, factors, received, mine))


def input_gradient(x, win, factors):
    vmem = pl.BlockSpec(memory_space=pltpu.VMEM)
    hbm = pl.BlockSpec(memory_space=pltpu.HBM)
    return pl.pallas_call(
        input_grad_kernel,
        out_shape=jax.ShapeDtypeStruct((1, LEN, D), bf16),
        in_specs=[hbm, hbm, vmem],
        out_specs=vmem,
        scratch_shapes=[
            pltpu.VMEM((LEN, D), bf16),
            pltpu.VMEM((D, 4 * D), bf16),
            pltpu.SemaphoreType.DMA((2,)),
        ],
        compiler_params=pltpu.CompilerParams(vmem_limit_bytes=8 << 20),
        name="input_gradient",
    )(*kept_in(pltpu.HBM, x, win), *kept_in(pltpu.VMEM, factors))


def group_sum_kernel(parts_ref, out_ref, total, ordered):
    summed = parts_ref[0].astype(f32)
    for g in range(1, GROUPS):
        summed += parts_ref[g].astype(f32)
    total[...] = summed
    for j in range(CHIPS):
        z = (FIRST_CHIP + j) % CHIPS
        ordered[PIECE * j : PIECE * j + 8, :] = total[8 * z : 8 * z + 8, :]
        ordered[PIECE * j + 8 : PIECE * j + 10, :] = total[pl.ds(256 + z, 2, stride=CHIPS), :]
    out_ref[...] = ordered[...].astype(bf16)


def group_sum(parts):
    vmem = pl.BlockSpec(memory_space=pltpu.VMEM)
    return pl.pallas_call(
        group_sum_kernel,
        out_shape=jax.ShapeDtypeStruct((CHIPS * PIECE, 128), bf16),
        in_specs=[vmem],
        out_specs=vmem,
        scratch_shapes=[pltpu.VMEM((ROWS, 128), f32), pltpu.VMEM((CHIPS * PIECE, 128), f32)],
        compiler_params=pltpu.CompilerParams(vmem_limit_bytes=8 << 20),
        name="group_sum",
    )(*kept_in(pltpu.VMEM, parts))


def chip_sum_kernel(parts_ref, out_ref, parts, copies):
    parts[...] = parts_ref[...].astype(f32)
    summed = parts[0:PIECE, :]
    for z in range(1, CHIPS):
        summed += parts[PIECE * z : PIECE * (z + 1), :]
    for g in range(GROUPS):
        copies[PIECE * g : PIECE * (g + 1), :] = summed
    out_ref[...] = copies[...].astype(bf16)


def chip_sum(parts):
    vmem = pl.BlockSpec(memory_space=pltpu.VMEM)
    return pl.pallas_call(
        chip_sum_kernel,
        out_shape=jax.ShapeDtypeStruct((GROUPS * PIECE, 128), bf16),
        in_specs=[vmem],
        out_specs=vmem,
        scratch_shapes=[
            pltpu.VMEM((CHIPS * PIECE, 128), f32),
            pltpu.VMEM((GROUPS * PIECE, 128), f32),
        ],
        compiler_params=pltpu.CompilerParams(vmem_limit_bytes=8 << 20),
        name="chip_sum",
    )(*kept_in(pltpu.VMEM, parts))


def finish_kernel(
    scale,
    swap_ref,
    home_ref,
    arrived_ref,
    parts_ref,
    out_ref,
    din_ref,
    dout_ref,
    parts,
):
    position = lax.axis_index("wide")
    chosen = swap_ref[lax.rem(position, CHIPS)] == 1

    @pl.when(chosen)
    def _():
        out_ref[...] = arrived_ref[...]

    @pl.when(jnp.logical_not(chosen))
    def _():
        out_ref[...] = home_ref[...]

    parts[...] = parts_ref[...].astype(f32) * scale
    for g in range(GROUPS):
        din_ref[:, g * 128 : (g + 1) * 128] = parts[PIECE * g : PIECE * g + 8, :]
        block, pair = g // 4, g % 4
        dout_ref[2 * pair : 2 * pair + 2, block * 128 : (block + 1) * 128] = parts[
            PIECE * g + 8 : PIECE * g + 10, :
        ]


def finish(scale, swaps, home, arrived, parts):
    vmem = pl.BlockSpec(memory_space=pltpu.VMEM)
    smem = pl.BlockSpec(memory_space=pltpu.SMEM)
    return pl.pallas_call(
        lambda *refs: finish_kernel(scale, *refs),
        out_shape=(
            jax.ShapeDtypeStruct((1, LEN, D), bf16),
            jax.ShapeDtypeStruct((8, 4 * D), f32),
            jax.ShapeDtypeStruct((8, D), f32),
        ),
        in_specs=[smem, vmem, vmem, vmem],
        out_specs=(vmem, vmem, vmem),
        scratch_shapes=[pltpu.VMEM((GROUPS * PIECE, 128), f32)],
        compiler_params=pltpu.CompilerParams(vmem_limit_bytes=8 << 20),
        name="finish",
    )(swaps, *kept_in(pltpu.VMEM, home, arrived, parts))


def exchanged(rows, count, axis, groups=None):
    pieces = rows.reshape(count, PIECE // 2, 2, 128)
    pieces = lax.all_to_all(pieces, axis, 0, 0, tiled=True, axis_index_groups=groups)
    return pieces.reshape(count * PIECE, 128)


def body(sequences, upstream, lengths, swap_table, input_weight, output_weight):
    wide = lax.axis_size("wide")
    half = wide // 2
    home, factors, mine = layer(
        lengths.reshape(wide), sequences, upstream, input_weight, output_weight
    )
    plane = [[(FIRST_GROUP + j) % GROUPS for j in range(GROUPS)]]
    same_core = [
        [2 * ((FIRST_CHIP + j) % CHIPS) + c for j in range(CHIPS)] for c in range(CORES)
    ]
    received = lax.ppermute(factors, "wide", [(i, i ^ 1) for i in range(wide)])
    arrived = lax.ppermute(home, "wide", [(i, (i + half) % wide) for i in range(wide)])
    chip = pair_half(factors, received, mine)
    parts = lax.all_to_all(chip, "grp", 0, 0, tiled=True, axis_index_groups=plane)
    input_grad = input_gradient(sequences, input_weight, factors)
    parts = group_sum(parts)
    parts = exchanged(parts, CHIPS, "wide", same_core)
    parts = chip_sum(parts)
    parts = exchanged(parts, GROUPS, "grp")
    scale = 1.0 / math.sqrt(LEN * wide * lax.axis_size("grp"))
    layer_out, total_in, total_out = finish(
        scale, swap_table.reshape(half), home, arrived, parts
    )
    return (layer_out, input_grad, total_in, total_out)


def solution(mesh):
    placed = (
        P(("grp", "wide"), None, None),
        P(("grp", "wide"), None, None),
        P("grp", None, None),
        P("grp", None, None),
        P(),
        P(),
    )
    return jax.shard_map(
        body,
        mesh=mesh,
        in_specs=placed,
        out_specs=(
            P(("grp", "wide"), None, None),
            P(("grp", "wide"), None, None),
            P("wide", None),
            P("wide", None),
        ),
        check_vma=False,
    )
```

```python
import math

import jax
import jax.numpy as jnp
from jax import lax
from jax.experimental import pallas as pl
from jax.experimental.pallas import tpu as pltpu
from jax.sharding import PartitionSpec as P


HEADS = 8
HEAD_DIM = 64
LEN = 128
D = 512
GROUPS = 16
CHIPS = 32
CORES = 2
ROWS = 320
PIECE = 10
FIRST_CHIP = 17
FIRST_GROUP = 10
epsilon = 1e-06
f32 = jnp.float32
bf16 = jnp.bfloat16


def nn(a, b):
    return lax.dot_general(a, b, (((1,), (0,)), ((), ())), preferred_element_type=f32)


def nt(a, b):
    return lax.dot_general(a, b, (((1,), (1,)), ((), ())), preferred_element_type=f32)


def tn(a, b):
    return lax.dot_general(a, b, (((0,), (0,)), ((), ())), preferred_element_type=f32)


def sigmoid(x):
    return 0.5 * jnp.tanh(0.5 * x) + 0.5


def place(group):
    return (group - FIRST_GROUP) % GROUPS


def layer_kernel(
    lengths_hbm,
    x_hbm,
    up_hbm,
    win_hbm,
    wout_hbm,
    home_ref,
    factors_ref,
    mine_ref,
    act_ref,
    slope_ref,
    wslope_ref,
    weights_ref,
    normed_t,
    gated_t,
    lengths_ref,
    x_ref,
    up_ref,
    win_ref,
    wout_ref,
    arrivals,
):
    parts = [(x_hbm.at[0], x_ref)]
    parts += [(win_hbm.at[:, pl.ds(j * D, D)], win_ref.at[:, pl.ds(j * D, D)]) for j in range(4)]
    parts += [(lengths_hbm, lengths_ref), (wout_hbm, wout_ref), (up_hbm.at[0], up_ref)]
    copies = [
        pltpu.make_async_copy(src, dst, arrivals.at[i]) for i, (src, dst) in enumerate(parts)
    ]
    for copy in copies:
        copy.start()
    position = lax.axis_index("wide")
    core = lax.rem(position, 2)
    copies[0].wait()
    x = x_ref[...].astype(f32)
    inverse = lax.rsqrt(jnp.mean(x * x, axis=-1, keepdims=True) + epsilon)
    unit = x * inverse
    normed = unit.astype(bf16)
    normed_t[...] = unit.astype(bf16).astype(f32).T.reshape(CHIPS, 16, LEN)
    for part in range(4):
        columns = pl.ds(part * D, D)
        copies[1 + part].wait()
        hidden = nn(normed, win_ref[:, columns])
        sig = sigmoid(hidden)
        activated = hidden * sig
        act_ref[:, columns] = activated.astype(bf16)
        slope_ref[:, columns] = sig + activated * (1.0 - sig)

    copies[5].wait()
    length = lengths_ref[position]
    query_at = lax.broadcasted_iota(jnp.int32, (LEN, LEN), 0)
    key_at = lax.broadcasted_iota(jnp.int32, (LEN, LEN), 1)
    allowed = (key_at <= query_at) & (key_at < length)
    first = lax.broadcasted_iota(jnp.int32, (LEN, LEN), 1) < HEAD_DIM

    def by_head(block):
        wide = block.astype(f32)
        return (
            jnp.where(first, wide, 0.0).astype(bf16),
            jnp.where(first, 0.0, wide).astype(bf16),
        )

    attended = []
    for pair in range(HEADS // 2):
        at = pair * 128
        queries = by_head(act_ref[:, 2 * D + at : 2 * D + at + 128])
        keys = act_ref[:, 3 * D + at : 3 * D + at + 128]
        values = by_head(act_ref[:, D + at : D + at + 128])
        for side in range(2):
            scores = nt(queries[side], keys) * HEAD_DIM**-0.5
            sig = sigmoid(scores)
            smooth = scores * sig
            slope = (sig + smooth * (1.0 - sig)) * HEAD_DIM**-0.5
            wslope_ref[2 * pair + side] = jnp.where(allowed, slope, 0.0)
            weights_ref[pair, side * LEN : (side + 1) * LEN, :] = jnp.where(
                allowed, smooth, 0.0
            ).astype(bf16)
        attended.append(
            nn(weights_ref[pair, :LEN, :], values[0]) + nn(weights_ref[pair, LEN:, :], values[1])
        )
    attended = jnp.concatenate(attended, axis=1)
    spread = lax.rsqrt(jnp.mean(attended * attended, axis=-1, keepdims=True) + epsilon)
    unit_attended = attended * spread
    gate = act_ref[:, :D].astype(f32)
    gated = (gate * unit_attended).astype(bf16)
    gated_t[...] = gated.astype(f32).T
    copies[6].wait()
    home_ref[0] = (x + nn(gated, wout_ref[...])).astype(bf16)

    copies[7].wait()
    alive = lax.broadcasted_iota(jnp.int32, (LEN, D), 0) < length
    masked = jnp.where(alive, up_ref[...].astype(f32), 0.0).astype(bf16)
    factors_ref[:, 4 * D : 5 * D] = masked
    gated_grad = nt(masked, wout_ref[...]).astype(bf16).astype(f32)
    factors_ref[:, :D] = (
        (gated_grad * unit_attended).astype(bf16).astype(f32) * slope_ref[:, :D]
    ).astype(bf16)
    unit_grad = gated_grad * gate
    overlap = jnp.mean(unit_grad * unit_attended, axis=-1, keepdims=True)
    attended_grad = spread * (unit_grad - unit_attended * overlap)

    for pair in range(HEADS // 2):
        at = pair * 128
        queries = by_head(act_ref[:, 2 * D + at : 2 * D + at + 128])
        keys = by_head(act_ref[:, 3 * D + at : 3 * D + at + 128])
        values = act_ref[:, D + at : D + at + 128]
        grads = by_head(attended_grad[:, at : at + 128])
        both = jnp.concatenate(grads, axis=0)
        weight_grads = nt(both, values)
        value_grad = tn(weights_ref[pair], both)
        score_grads = (
            weight_grads * wslope_ref[2 * pair : 2 * pair + 2].reshape(2 * LEN, LEN)
        ).astype(bf16)
        query_grad = nn(score_grads[:LEN], keys[0]) + nn(score_grads[LEN:], keys[1])
        key_grad = tn(score_grads, jnp.concatenate(queries, axis=0))
        for start, grad in ((D, value_grad), (2 * D, query_grad), (3 * D, key_grad)):
            columns = pl.ds(start + at, 128)
            factors_ref[:, columns] = (grad * slope_ref[:, columns]).astype(bf16)

    def columns_of(side):
        rows = pl.ds(pl.multiple_of(side * 8, 8), 8)
        normed_part = normed_t[:, rows, :].reshape(256, LEN).astype(bf16)
        gated_part = jnp.concatenate(
            [gated_t[pl.ds(side * 8 + i, CHIPS, stride=16), :] for i in range(8)], axis=0
        ).astype(bf16)
        return (normed_part[:128], normed_part[128:], gated_part[:128], gated_part[128:])

    for i, block in enumerate(columns_of(1 - core)):
        factors_ref[:, 5 * D + 128 * i : 5 * D + 128 * (i + 1)] = block
    for i, block in enumerate(columns_of(core)):
        mine_ref[128 * i : 128 * (i + 1), :] = block


def pair_kernel(factors_ref, received_ref, mine_ref, out_hbm, out_ref, sent):
    theirs = [received_ref[:, 5 * D + 128 * i : 5 * D + 128 * (i + 1)] for i in range(4)]
    theirs = jnp.concatenate(theirs, axis=0)
    left = jnp.concatenate([mine_ref[...], theirs], axis=1)

    def right(start, width):
        columns = pl.ds(start, width)
        return jnp.concatenate([factors_ref[:, columns], received_ref[:, columns]], axis=0)

    grads_out = nn(left[256:], right(4 * D, D)).astype(bf16)
    copies = []
    for block in range(4):
        grads = nn(left[:256], right(block * D, D)).astype(bf16)
        for j in range(4):
            at = place(4 * block + j)
            out_ref[at, 0:256, :] = grads[:, j * 128 : (j + 1) * 128]
            out_ref[at, 256:320, :] = grads_out[
                j * 64 : (j + 1) * 64, block * 128 : (block + 1) * 128
            ]
            copies.append(
                pltpu.make_async_copy(out_ref.at[at], out_hbm.at[at], sent.at[4 * block + j])
            )
            copies[-1].start()
    for copy in copies:
        copy.wait()


def input_grad_kernel(x_hbm, win_hbm, factors_ref, xgrad_ref, x_ref, win_ref, arrivals):
    copies = [
        pltpu.make_async_copy(x_hbm.at[0], x_ref, arrivals.at[0]),
        pltpu.make_async_copy(win_hbm, win_ref, arrivals.at[1]),
    ]
    for copy in copies:
        copy.start()
    copies[0].wait()
    x = x_ref[...].astype(f32)
    inverse = lax.rsqrt(jnp.mean(x * x, axis=-1, keepdims=True) + epsilon)
    unit = x * inverse
    copies[1].wait()
    unit_grad = nt(factors_ref[:, : 4 * D], win_ref[...])
    overlap = jnp.mean(unit_grad * unit, axis=-1, keepdims=True)
    xgrad_ref[0] = (
        factors_ref[:, 4 * D : 5 * D].astype(f32) + inverse * (unit_grad - unit * overlap)
    ).astype(bf16)


def kept_in(space, *arrays):
    return [pltpu.with_memory_space_constraint(array, space) for array in arrays]


def layer(lengths, x, up, win, wout):
    vmem = pl.BlockSpec(memory_space=pltpu.VMEM)
    hbm = pl.BlockSpec(memory_space=pltpu.HBM)
    shapes = [(1, LEN, D), (LEN, 6 * D), (512, LEN)]
    return pl.pallas_call(
        layer_kernel,
        out_shape=[jax.ShapeDtypeStruct(shape, bf16) for shape in shapes],
        in_specs=[hbm] * 5,
        out_specs=[vmem] * 3,
        scratch_shapes=[
            pltpu.VMEM((LEN, 4 * D), bf16),
            pltpu.VMEM((LEN, 4 * D), f32),
            pltpu.VMEM((HEADS, LEN, LEN), f32),
            pltpu.VMEM((HEADS // 2, 2 * LEN, LEN), bf16),
            pltpu.VMEM((CHIPS, 16, LEN), f32),
            pltpu.VMEM((D, LEN), f32),
            pltpu.SMEM((2 * CHIPS,), jnp.int32),
            pltpu.VMEM((LEN, D), bf16),
            pltpu.VMEM((LEN, D), bf16),
            pltpu.VMEM((D, 4 * D), bf16),
            pltpu.VMEM((D, D), bf16),
            pltpu.SemaphoreType.DMA((8,)),
        ],
        compiler_params=pltpu.CompilerParams(vmem_limit_bytes=24 << 20),
        name="layer",
    )(*kept_in(pltpu.HBM, lengths, x, up, win, wout))


def pair_half(factors, received, mine):
    vmem = pl.BlockSpec(memory_space=pltpu.VMEM)
    shape = (GROUPS, ROWS, 128)
    return pl.pallas_call(
        pair_kernel,
        out_shape=jax.ShapeDtypeStruct(shape, bf16),
        in_specs=[vmem] * 3,
        out_specs=pl.BlockSpec(memory_space=pltpu.HBM),
        scratch_shapes=[pltpu.VMEM(shape, bf16), pltpu.SemaphoreType.DMA((GROUPS,))],
        compiler_params=pltpu.CompilerParams(vmem_limit_bytes=12 << 20),
        name="pair_half",
    )(*kept_in(pltpu.VMEM, factors, received, mine))


def input_gradient(x, win, factors):
    vmem = pl.BlockSpec(memory_space=pltpu.VMEM)
    hbm = pl.BlockSpec(memory_space=pltpu.HBM)
    return pl.pallas_call(
        input_grad_kernel,
        out_shape=jax.ShapeDtypeStruct((1, LEN, D), bf16),
        in_specs=[hbm, hbm, vmem],
        out_specs=vmem,
        scratch_shapes=[
            pltpu.VMEM((LEN, D), bf16),
            pltpu.VMEM((D, 4 * D), bf16),
            pltpu.SemaphoreType.DMA((2,)),
        ],
        compiler_params=pltpu.CompilerParams(vmem_limit_bytes=8 << 20),
        name="input_gradient",
    )(*kept_in(pltpu.HBM, x, win), *kept_in(pltpu.VMEM, factors))


def group_sum_kernel(parts_ref, out_ref, total, ordered):
    summed = parts_ref[0].astype(f32)
    for g in range(1, GROUPS):
        summed += parts_ref[g].astype(f32)
    total[...] = summed
    for j in range(CHIPS):
        z = (FIRST_CHIP + j) % CHIPS
        ordered[PIECE * j : PIECE * j + 8, :] = total[8 * z : 8 * z + 8, :]
        ordered[PIECE * j + 8 : PIECE * j + 10, :] = total[pl.ds(256 + z, 2, stride=CHIPS), :]
    out_ref[...] = ordered[...].astype(bf16)


def group_sum(parts):
    vmem = pl.BlockSpec(memory_space=pltpu.VMEM)
    return pl.pallas_call(
        group_sum_kernel,
        out_shape=jax.ShapeDtypeStruct((CHIPS * PIECE, 128), bf16),
        in_specs=[vmem],
        out_specs=vmem,
        scratch_shapes=[pltpu.VMEM((ROWS, 128), f32), pltpu.VMEM((CHIPS * PIECE, 128), f32)],
        compiler_params=pltpu.CompilerParams(vmem_limit_bytes=8 << 20),
        name="group_sum",
    )(*kept_in(pltpu.VMEM, parts))


def chip_sum_kernel(parts_ref, out_ref, parts, copies):
    parts[...] = parts_ref[...].astype(f32)
    summed = parts[0:PIECE, :]
    for z in range(1, CHIPS):
        summed += parts[PIECE * z : PIECE * (z + 1), :]
    for g in range(GROUPS):
        copies[PIECE * g : PIECE * (g + 1), :] = summed
    out_ref[...] = copies[...].astype(bf16)


def chip_sum(parts):
    vmem = pl.BlockSpec(memory_space=pltpu.VMEM)
    return pl.pallas_call(
        chip_sum_kernel,
        out_shape=jax.ShapeDtypeStruct((GROUPS * PIECE, 128), bf16),
        in_specs=[vmem],
        out_specs=vmem,
        scratch_shapes=[
            pltpu.VMEM((CHIPS * PIECE, 128), f32),
            pltpu.VMEM((GROUPS * PIECE, 128), f32),
        ],
        compiler_params=pltpu.CompilerParams(vmem_limit_bytes=8 << 20),
        name="chip_sum",
    )(*kept_in(pltpu.VMEM, parts))


def select_kernel(swap_ref, home_ref, arrived_ref, out_ref):
    position = lax.axis_index("wide")
    chosen = swap_ref[lax.rem(position, CHIPS)] == 1

    @pl.when(chosen)
    def _():
        out_ref[...] = arrived_ref[...]

    @pl.when(jnp.logical_not(chosen))
    def _():
        out_ref[...] = home_ref[...]


def selected(swaps, home, arrived):
    vmem = pl.BlockSpec(memory_space=pltpu.VMEM)
    smem = pl.BlockSpec(memory_space=pltpu.SMEM)
    return pl.pallas_call(
        select_kernel,
        out_shape=jax.ShapeDtypeStruct((1, LEN, D), bf16),
        in_specs=[smem, vmem, vmem],
        out_specs=vmem,
        compiler_params=pltpu.CompilerParams(vmem_limit_bytes=8 << 20),
        name="selected",
    )(swaps, *kept_in(pltpu.VMEM, home, arrived))


def finish_kernel(scale, parts_ref, din_ref, dout_ref, parts):
    parts[...] = parts_ref[...].astype(f32) * scale
    for g in range(GROUPS):
        din_ref[:, g * 128 : (g + 1) * 128] = parts[PIECE * g : PIECE * g + 8, :]
        block, pair = g // 4, g % 4
        dout_ref[2 * pair : 2 * pair + 2, block * 128 : (block + 1) * 128] = parts[
            PIECE * g + 8 : PIECE * g + 10, :
        ]


def finish(scale, parts):
    vmem = pl.BlockSpec(memory_space=pltpu.VMEM)
    return pl.pallas_call(
        lambda *refs: finish_kernel(scale, *refs),
        out_shape=(
            jax.ShapeDtypeStruct((8, 4 * D), f32),
            jax.ShapeDtypeStruct((8, D), f32),
        ),
        in_specs=[vmem],
        out_specs=(vmem, vmem),
        scratch_shapes=[pltpu.VMEM((GROUPS * PIECE, 128), f32)],
        compiler_params=pltpu.CompilerParams(vmem_limit_bytes=8 << 20),
        name="finish",
    )(*kept_in(pltpu.VMEM, parts))


def exchanged(rows, count, axis, groups=None):
    pieces = rows.reshape(count, PIECE // 2, 2, 128)
    pieces = lax.all_to_all(pieces, axis, 0, 0, tiled=True, axis_index_groups=groups)
    return pieces.reshape(count * PIECE, 128)


def body(sequences, upstream, lengths, swap_table, input_weight, output_weight):
    wide = lax.axis_size("wide")
    half = wide // 2
    home, factors, mine = layer(
        lengths.reshape(wide), sequences, upstream, input_weight, output_weight
    )
    plane = [[(FIRST_GROUP + j) % GROUPS for j in range(GROUPS)]]
    same_core = [
        [2 * ((FIRST_CHIP + j) % CHIPS) + c for j in range(CHIPS)] for c in range(CORES)
    ]
    received = lax.ppermute(factors, "wide", [(i, i ^ 1) for i in range(wide)])
    arrived = lax.ppermute(home, "wide", [(i, (i + half) % wide) for i in range(wide)])
    chip = pair_half(factors, received, mine)
    parts = lax.all_to_all(chip, "grp", 0, 0, tiled=True, axis_index_groups=plane)
    input_grad = input_gradient(sequences, input_weight, factors)
    parts = group_sum(parts)
    parts = exchanged(parts, CHIPS, "wide", same_core)
    parts = chip_sum(parts)
    layer_out = selected(swap_table.reshape(half), home, arrived)
    parts = exchanged(parts, GROUPS, "grp")
    scale = 1.0 / math.sqrt(LEN * wide * lax.axis_size("grp"))
    total_in, total_out = finish(scale, parts)
    return (layer_out, input_grad, total_in, total_out)


def solution(mesh):
    placed = (
        P(("grp", "wide"), None, None),
        P(("grp", "wide"), None, None),
        P("grp", None, None),
        P("grp", None, None),
        P(),
        P(),
    )
    return jax.shard_map(
        body,
        mesh=mesh,
        in_specs=placed,
        out_specs=(
            P(("grp", "wide"), None, None),
            P(("grp", "wide"), None, None),
            P("wide", None),
            P("wide", None),
        ),
        check_vma=False,
    )
```
